256 devices in a mesh: tok: 64 (over z, x, core), exp: 4 (over y).
Axes of the slice: x: 4, y: 4, z: 8, core: 2. Of those that a mesh axis runs over, the one named last changes fastest.
Arguments:
- tokens: bfloat16 [131072, 7168], P('tok', 'exp'), may hold values from -6 to 6
- gate_weight: bfloat16 [7168, 256], P('exp'), may hold values from -0.0625 to 0.0625
- expert_ids: int32 [131072, 8], P('tok'), may hold values from 0 to 255, all different within a row
- expert_bias: float32 [256], P('exp'), may hold values from -0.002 to 0.002
Outputs:
- affinities: float32 [131072, 256], P('tok', 'exp')
- weights: float32 [131072, 8], P('tok')
- load: float32 [256], replicated
- new_bias: float32 [256], replicated
The draws below stay inside these ranges and needn't reach their ends.
All inputs are finite; a program needn't handle non-finite values.
Results may differ from the reference program's by a relative error of at most 0.0003.
Values may be sent and summed in bfloat16 or wider, within the bound.
A program may use at most 64 MiB of HBM per device.

```python
import jax
import jax.numpy as jnp
from jax import lax

D = 7168
E = 256
TOPK = 8
TOKENS = 131072


def block_scale(rng, extent, shards, low, high):
    def one(axis_at, blocks):
        draws = jax.random.uniform(jax.random.fold_in(jax.random.fold_in(rng, 6), axis_at), (blocks,), jnp.float32, low / len(shards), high / len(shards))
        return jnp.repeat(jnp.exp(draws), extent[axis_at] // blocks).reshape((-1,) + (1,) * (len(extent) - axis_at - 1))

    loudness = one(*shards[0])
    for cut in shards[1:]:
        loudness = loudness * one(*cut)
    return loudness


def picks_of(stream_key, rows, count, top, lift):
    ranking = jax.random.permutation(jax.random.fold_in(stream_key, 1), count)
    boost = ranking
    for power in range(3):
        boost = boost * boost // count
    boost = boost * lift // count
    tickets = jax.random.randint(jax.random.fold_in(stream_key, 2), (rows, count), 0, 4096) + boost
    holders = jax.random.permutation(jax.random.fold_in(stream_key, 3), rows)[jnp.arange(count) % rows]
    tickets = jnp.where(jnp.arange(rows)[:, None] == holders[None, :], 1 << 14, tickets)
    priority = tickets * count + jnp.arange(count)
    return lax.top_k(priority.astype(jnp.int32), top)[1].astype(jnp.int32)


def gaussian(own_key, shape, deviation, bound, shards=(), kind=jnp.bfloat16):
    loudness = block_scale(own_key, shape, shards, -0.22, 0.18) if shards else 1.0
    values = jax.random.normal(own_key, shape, jnp.float32) * deviation * loudness
    return jnp.minimum(jnp.maximum(values, -bound), bound).astype(kind)


def setup_inputs(seed: int = 0) -> dict:
    key_of = jax.random.split(jax.random.key(seed), 5)
    tokens = gaussian(key_of[0], (TOKENS, D), 1.0, 6.0, ((0, 64), (1, 4)))
    gate_weight = gaussian(key_of[1], (D, E), D ** -0.5, 0.0625, ((0, 4),))
    expert_ids = picks_of(key_of[2], TOKENS, E, TOPK, 512)
    expert_bias = jnp.clip(jax.random.uniform(key_of[3], (E,), jnp.float32, -0.002, 0.002) * block_scale(key_of[3], (E,), ((0, 4),), -0.4, 0.0), -0.002, 0.002)
    return {"tokens": tokens, "gate_weight": gate_weight, "expert_ids": expert_ids, "expert_bias": expert_bias}


def reference(tokens, gate_weight, expert_ids, expert_bias):
    logits = jnp.dot(tokens, gate_weight, preferred_element_type=jnp.float32)
    affinities = jax.nn.sigmoid(logits)
    chosen = jnp.take_along_axis(affinities, expert_ids, axis=1)
    weights = 2.5 * chosen / jnp.sum(chosen, axis=1, keepdims=True)
    numbers = jnp.arange(E, dtype=jnp.int32)
    load = jnp.sum((expert_ids[:, :, None] == numbers[None, None, :]).astype(jnp.float32), axis=(0, 1))
    target = jnp.float32(TOKENS * TOPK)
    new_bias = expert_bias + 0.001 * jnp.sign(target - jnp.float32(E) * load)
    return affinities, weights, load, new_bias
```

```python
import functools

import jax
import jax.numpy as jnp
from jax import lax
from jax.experimental import pallas as pl
from jax.experimental.pallas import tpu as pltpu
from jax.sharding import Mesh
from jax.sharding import PartitionSpec as P

TOK = ("tok_0", "tok_1", "tok_2")
MESH = pl.DeviceIdType.MESH
F32 = jnp.float32
BF16 = jnp.bfloat16
I32 = jnp.int32
I16 = jnp.int16

STEPS = 3800.0
KNEE = 0.25


def encode(x):
    grade = jnp.log(jnp.abs(x) * (1.0 / KNEE) + 1.0) * STEPS + 0.5
    return jnp.where(x < 0.0, -grade, grade).astype(I32)


def decode(code):
    grade = code.astype(I32).astype(F32)
    size = jnp.exp(jnp.abs(grade) * (1.0 / STEPS)) * KNEE - KNEE
    return jnp.where(grade < 0.0, -size, size)


def sigmoid(x):
    return 1.0 / (1.0 + jnp.exp(-x))


def kernel(
    sizes, x_hbm, w_hbm, ids_hbm, bias_hbm, aff_ref, wts_ref, load_ref, new_ref,
    x_v, w_v, wt_v, ids_v, bias_v, p_v, acc_v,
    sa1, sb1, sa2, sb2, sc1, sc2, ra1, rb1, ra2, rb2, rc1, rc2,
    hot_hi, hot_lo, d0, d1, dr1, dr2, b0, b1, br1, br2,
    x_sem, in_sem, ss, rs, d1_ss, d1_rs, d2_ss, d2_rs, b_ss, b_rs, near,
):
    nz, nx, nc, chunks, width, target = sizes
    own = 64
    half = own // 2
    z, xx, core, m = (lax.axis_index(a) for a in (*TOK, "exp"))
    mate = m + 1 - 2 * (m % 2)
    cross = 3 - m
    group = nx * nc
    place = xx * nc + core

    def sibling(r):
        peer = (place + r) % group
        return {"tok_1": peer // nc, "tok_2": peer % nc}

    def along(r):
        return {"tok_0": (z + r) % nz}

    def x_copy(c):
        return pltpu.make_async_copy(
            x_hbm.at[pl.ds(pl.multiple_of(c * width, width), width), :], x_v.at[c], x_sem.at[c]
        )

    ids_copy = pltpu.make_async_copy(ids_hbm, ids_v, in_sem.at[0])
    w_copy = pltpu.make_async_copy(w_hbm, w_v, in_sem.at[1])
    bias_copy = pltpu.make_async_copy(bias_hbm, bias_v, in_sem.at[2])
    ids_copy.start()
    w_copy.start()
    bias_copy.start()
    for c in range(chunks):
        x_copy(c).start()

    barrier = pltpu.get_barrier_semaphore()
    steps = sorted({s % nz for s in (1, 2, -1, -2)} - {0})
    partners = [{"exp": mate}, {"exp": cross}]
    partners += [sibling(r) for r in range(1, group)]
    partners += [along(s) for s in steps]
    for partner in partners:
        pl.semaphore_signal(barrier, inc=1, device_id=partner, device_id_type=MESH)

    ids_copy.wait()
    digits = lax.broadcasted_iota(I32, (16, 8, width), 0)

    def count(c, total):
        ids = ids_v[:, pl.ds(pl.multiple_of(c * width, width), width)]
        hi, lo = ids >> 4, ids & 15
        one_hi = jnp.where(hi[None] == digits, 1.0, 0.0).reshape(128, width).astype(BF16)
        one_lo = jnp.where(lo[None] == digits, 1.0, 0.0).reshape(128, width).astype(BF16)
        return total + lax.dot_general(
            one_hi, one_lo, (((1,), (1,)), ((), ())), preferred_element_type=F32
        )

    pairs = lax.fori_loop(0, chunks, count, jnp.zeros((128, 128), F32))
    row = lax.broadcasted_iota(I32, (128, 128), 0)
    col = lax.broadcasted_iota(I32, (128, 128), 1)
    by_slot = jnp.where(row % 8 == col % 8, pairs, 0.0).reshape(16, 8, 128).sum(axis=1)
    fold = jnp.where(row // 8 == col % 16, 1.0, 0.0).astype(BF16)
    upper = jnp.floor(by_slot * (1.0 / 64.0))
    lower = by_slot - 64.0 * upper
    counts = 64.0 * jnp.dot(upper.astype(BF16), fold, preferred_element_type=F32) + jnp.dot(
        lower.astype(BF16), fold, preferred_element_type=F32
    )
    sub = lax.broadcasted_iota(I32, (8, 128), 0)
    lane = lax.broadcasted_iota(I32, (8, 128), 1)
    pick = lane // 16 == sub
    first = jnp.sum(jnp.where(pick, counts[:8], 0.0), axis=0, keepdims=True)
    second = jnp.sum(jnp.where(pick, counts[8:], 0.0), axis=0, keepdims=True)
    d0[...] = jnp.where(sub == 0, first, jnp.where(sub == 1, second, 0.0))

    bias_copy.wait()
    mine = bias_v[...]
    mine = jnp.broadcast_to(jnp.concatenate([mine, mine], axis=1), (8, 128))
    b0[...] = jnp.where((sub == m // 2) & (lane // own == m % 2), mine, 0.0)

    w_copy.wait()
    wt_v[...] = w_v[...].T

    low_a = jnp.where(m % 3 == 0, 1, 0)
    low_b = jnp.where(m < 2, 2, 0)
    pos_a = jnp.where(m < 2, 0, 1)
    pos_b = m % 2

    def part(c, block, second_half):
        return p_v[c, pl.ds(pl.multiple_of(block * own + second_half * half, half), half), :]

    def compute(c):
        x_copy(c).wait()
        p_v[c] = lax.dot_general(
            wt_v[...], x_v[c], (((1,), (1,)), ((), ())), preferred_element_type=F32
        )
        sa1[c, :half] = encode(part(c, low_a, 0)).astype(I16)
        sa1[c, half:] = encode(part(c, 3 - low_a, 0)).astype(I16)
        sb1[c, :half] = encode(part(c, low_b, 1)).astype(I16)
        sb1[c, half:] = encode(part(c, low_b + 1, 1)).astype(I16)
        ids = ids_v[:, pl.ds(pl.multiple_of(c * width, width), width)]
        tile, within = ids >> 3, ids & 7
        chosen = jnp.zeros((8, width), F32)
        for k in range(4 * own // 8):
            rows = p_v[c, 8 * k : 8 * k + 8, :]
            got = jnp.take_along_axis(rows, within, axis=0, mode="promise_in_bounds")
            chosen = jnp.where(tile == k, got, chosen)
        code = encode(chosen)
        sc1[c] = jnp.concatenate(
            [code[:, 128 * i : 128 * (i + 1)] for i in range(width // 128)], axis=0
        ).astype(I16)

    def remote(src, dst, c, kind, partner):
        return pltpu.make_async_remote_copy(
            src_ref=src.at[c],
            dst_ref=dst.at[c],
            send_sem=ss.at[kind, c],
            recv_sem=rs.at[kind, c],
            device_id={"exp": partner},
            device_id_type=MESH,
        )

    def even(c):
        return jnp.where(c % 2 == 0, mate, cross)

    def odd(c):
        return jnp.where(c % 2 == 0, cross, mate)

    def copies_1(c):
        return (
            remote(sa1, ra1, c, 0, mate),
            remote(sb1, rb1, c, 1, cross),
            remote(sc1, rc1, c, 2, even(c)),
        )

    def copies_2(c):
        return (
            remote(sa2, ra2, c, 3, cross),
            remote(sb2, rb2, c, 4, mate),
            remote(sc2, rc2, c, 5, odd(c)),
        )

    def send(copies):
        for copy in copies:
            copy.start()

    def count_copies_1(r):
        return pltpu.make_async_remote_copy(
            src_ref=d0, dst_ref=dr1.at[r - 1], send_sem=d1_ss.at[r - 1], recv_sem=d1_rs.at[r - 1],
            device_id=sibling(r), device_id_type=MESH,
        )

    def count_copies_2(r):
        return pltpu.make_async_remote_copy(
            src_ref=d1, dst_ref=dr2.at[r - 1], send_sem=d2_ss.at[r - 1], recv_sem=d2_rs.at[r - 1],
            device_id=along(r), device_id_type=MESH,
        )

    def bias_copy_to(src, dst, i, partner):
        return pltpu.make_async_remote_copy(
            src_ref=src, dst_ref=dst, send_sem=b_ss.at[i], recv_sem=b_rs.at[i],
            device_id={"exp": partner}, device_id_type=MESH,
        )

    compute(0)
    pl.semaphore_wait(barrier, len(partners))
    send(copies_1(0))
    for r in range(1, group):
        count_copies_1(r).start()
    bias_copy_to(b0, br1, 0, mate).start()
    far = sorted({s % nz for s in (2, -2)} - {0})
    for s in far:
        pl.semaphore_signal(near, inc=1, device_id=along(s), device_id_type=MESH)

    @pl.loop(1, chunks)
    def _(c):
        compute(c)
        send(copies_1(c))

    for r in range(1, group):
        count_copies_1(r).wait_recv()
    d1[...] = sum((dr1[r - 1] for r in range(1, group)), d0[...])
    bias_copy_to(b0, br1, 0, mate).wait_recv()
    b1[...] = b0[...] + br1[...]
    pl.semaphore_wait(near, len(far))
    for r in range(1, nz):
        count_copies_2(r).start()
    bias_copy_to(b1, br2, 1, cross).start()

    @pl.loop(0, chunks)
    def _(c):
        for copy in copies_1(c):
            copy.wait_recv()
        at_a = pl.multiple_of(pos_a * half, half)
        at_b = pl.multiple_of(pos_b * half, half)
        off_a = pl.multiple_of((1 - pos_a) * half, half)
        off_b = pl.multiple_of((1 - pos_b) * half, half)
        sa2[c] = encode(part(c, cross, 0) + decode(ra1[c, pl.ds(off_a, half), :])).astype(I16)
        sb2[c] = encode(part(c, mate, 1) + decode(rb1[c, pl.ds(off_b, half), :])).astype(I16)
        sc2[c] = encode(decode(sc1[c]) + decode(rc1[c])).astype(I16)
        acc_v[c, :half] = part(c, m, 0) + decode(ra1[c, pl.ds(at_a, half), :])
        acc_v[c, half:] = part(c, m, 1) + decode(rb1[c, pl.ds(at_b, half), :])
        send(copies_2(c))

    for r in range(1, nz):
        count_copies_2(r).wait_recv()
    bias_copy_to(b1, br2, 1, cross).wait_recv()
    load = sum((dr2[r - 1] for r in range(1, nz)), d1[...])
    gap = target - (4.0 * own) * load
    sign = jnp.where(gap > 0.0, 1.0, jnp.where(gap < 0.0, -1.0, 0.0))
    new_bias = (b1[...] + br2[...]) + 0.001 * sign
    for i in range(2):
        load_ref[:, 128 * i : 128 * (i + 1)] = load[i : i + 1]
        new_ref[:, 128 * i : 128 * (i + 1)] = new_bias[i : i + 1]

    @pl.loop(0, chunks)
    def _(c):
        for copy in copies_2(c):
            copy.wait_recv()
        at = pl.multiple_of(c * width, width)
        aff_ref[:half, pl.ds(at, width)] = sigmoid(acc_v[c, :half] + decode(ra2[c]))
        aff_ref[half:, pl.ds(at, width)] = sigmoid(acc_v[c, half:] + decode(rb2[c]))
        chosen = sigmoid(decode(sc2[c]) + decode(rc2[c]))
        for i in range(width // 128):
            values = chosen[8 * i : 8 * i + 8]
            total = jnp.sum(values, axis=0, keepdims=True)
            wts_ref[:, pl.ds(pl.multiple_of(at + 128 * i, 128), 128)] = 2.5 * values / total

    @pl.loop(0, chunks)
    def _(c):
        for copy in (*copies_1(c), *copies_2(c)):
            copy.wait_send()

    for r in range(1, group):
        count_copies_1(r).wait_send()
    for r in range(1, nz):
        count_copies_2(r).wait_send()
    bias_copy_to(b0, br1, 0, mate).wait_send()
    bias_copy_to(b1, br2, 1, cross).wait_send()


def hand_out(*refs):
    count = len(refs) // 2
    copies = [
        pltpu.make_async_copy(refs[i], refs[count + i], refs[-1].at[i]) for i in range(count)
    ]
    for copy in copies:
        copy.start()
    for copy in copies:
        copy.wait()


def local(shape, tokens, gate_weight, expert_ids, expert_bias):
    nz, nx, nc = shape
    rows, depth = tokens.shape
    experts = gate_weight.shape[1]
    slots = expert_ids.shape[1]
    width = 256
    chunks = rows // width
    own = experts // 4
    target = float(rows * nz * nx * nc * slots)
    sizes = (nz, nx, nc, chunks, width, target)
    dma = pltpu.SemaphoreType.DMA
    big = pltpu.VMEM((chunks, own, width), I16)
    small = pltpu.VMEM((chunks, own // 2, width), I16)
    few = pltpu.VMEM((chunks, 16, 128), I16)
    tile = pltpu.VMEM((8, 128), F32)
    group = nx * nc
    made = pl.pallas_call(
        functools.partial(kernel, sizes),
        out_shape=(
            pltpu.VMEM((own, rows), F32),
            pltpu.VMEM((slots, rows), F32),
            pltpu.VMEM((1, experts), F32),
            pltpu.VMEM((1, experts), F32),
        ),
        in_specs=[pl.BlockSpec(memory_space=pltpu.HBM)] * 4,
        out_specs=(pl.BlockSpec(memory_space=pltpu.VMEM),) * 4,
        scratch_shapes=[
            pltpu.VMEM((chunks, width, depth), BF16),
            pltpu.VMEM((depth, experts), BF16),
            pltpu.VMEM((experts, depth), BF16),
            pltpu.VMEM((slots, rows), I32),
            pltpu.VMEM((1, own), F32),
            pltpu.VMEM((chunks, experts, width), F32),
            pltpu.VMEM((chunks, own, width), F32),
            big, big, small, small, few, few, big, big, small, small, few, few,
            pltpu.VMEM((128, width), BF16), pltpu.VMEM((128, width), BF16),
            tile, tile,
            pltpu.VMEM((max(group - 1, 1), 8, 128), F32), pltpu.VMEM((max(nz - 1, 1), 8, 128), F32),
            tile, tile, tile, tile,
            dma((chunks,)), dma((3,)), dma((6, chunks)), dma((6, chunks)),
            dma((max(group - 1, 1),)), dma((max(group - 1, 1),)),
            dma((max(nz - 1, 1),)), dma((max(nz - 1, 1),)),
            dma((2,)), dma((2,)), pltpu.SemaphoreType.REGULAR,
        ],
        compiler_params=pltpu.CompilerParams(
            collective_id=0, has_side_effects=True, vmem_limit_bytes=66300000
        ),
        name="router",
    )(tokens, gate_weight, expert_ids.T, expert_bias.reshape(1, own))
    aff, wts, load, new = pl.pallas_call(
        hand_out,
        out_shape=tuple(jax.ShapeDtypeStruct(a.shape, a.dtype) for a in made),
        in_specs=[pl.BlockSpec(memory_space=pltpu.VMEM)] * 4,
        out_specs=(pl.BlockSpec(memory_space=pltpu.HBM),) * 4,
        scratch_shapes=[dma((4,))],
        compiler_params=pltpu.CompilerParams(vmem_limit_bytes=2**20),
        name="hand_out",
    )(*made)
    return aff.T, wts.T, load.reshape(experts), new.reshape(experts)


def solution(mesh):
    shape = (8, 4, 2)
    split = Mesh(mesh.devices.reshape(*shape, mesh.shape["exp"]), (*TOK, "exp"))
    in_specs = (P(TOK, "exp"), P("exp", None), P(TOK, None), P("exp"))
    out_specs = (P(TOK, "exp"), P(TOK, None), P(), P())
    return jax.shard_map(
        functools.partial(local, shape),
        mesh=split, in_specs=in_specs, out_specs=out_specs, check_vma=False,
    )
```

```python
import functools

import jax
import jax.numpy as jnp
from jax import lax
from jax.experimental import pallas as pl
from jax.experimental.pallas import tpu as pltpu
from jax.sharding import Mesh
from jax.sharding import PartitionSpec as P

TOK = ("tok_0", "tok_1", "tok_2")
MESH = pl.DeviceIdType.MESH
F32 = jnp.float32
BF16 = jnp.bfloat16
I32 = jnp.int32
I16 = jnp.int16

STEPS = 3800.0
KNEE = 0.25


def encode(x):
    grade = jnp.log(jnp.abs(x) * (1.0 / KNEE) + 1.0) * STEPS + 0.5
    return jnp.where(x < 0.0, -grade, grade).astype(I32)


def decode(code):
    grade = code.astype(I32).astype(F32)
    size = jnp.exp(jnp.abs(grade) * (1.0 / STEPS)) * KNEE - KNEE
    return jnp.where(grade < 0.0, -size, size)


def sigmoid(x):
    return 1.0 / (1.0 + jnp.exp(-x))


def kernel(
    sizes, x_hbm, w_hbm, ids_hbm, bias_hbm, aff_ref, wts_ref, load_ref, new_ref,
    x_v, w_v, wt_v, ids_v, bias_v, p_v, acc_v,
    sa1, sb1, sa2, sb2, sc1, sc2, ra1, rb1, ra2, rb2, rc1, rc2,
    hot_hi, hot_lo, d0, d1, u1, u2, total, near_by, above, below, b0, b1, br1, br2,
    x_sem, in_sem, ss, rs, near_ss, near_rs, down_ss, down_rs, up_ss, up_rs, b_ss, b_rs, o_sem, wave, crest_1, crest_2,
):
    nz, nx, nc, chunks, width, target = sizes
    own = 64
    half = own // 2
    z, xx, core, m = (lax.axis_index(a) for a in (*TOK, "exp"))
    even_y = lax.rem(m, 2) == 0
    mate = jnp.where(even_y, m + 1, m - 1)
    cross = 3 - m
    lead = core == 1
    siblings = [(dx, dc) for dx in range(nx) for dc in range(nc)][1:]

    def turned(at, by, length):
        there = at + by
        return jnp.where(there >= length, there - length, there)

    def sibling(r):
        dx, dc = siblings[r]
        return {"tok_1": turned(xx, dx, nx), "tok_2": turned(core, dc, nc)}

    def x_copy(c):
        return pltpu.make_async_copy(
            x_hbm.at[pl.ds(pl.multiple_of(c * width, width), width), :], x_v.at[c], x_sem.at[c]
        )

    ids_copy = pltpu.make_async_copy(ids_hbm, ids_v, in_sem.at[0])
    w_copy = pltpu.make_async_copy(w_hbm, w_v, in_sem.at[1])
    bias_copy = pltpu.make_async_copy(bias_hbm, bias_v, in_sem.at[2])
    ids_copy.start()
    w_copy.start()
    x_copy(0).start()
    bias_copy.start()

    barrier = pltpu.get_barrier_semaphore()

    def greet(partner):
        pl.semaphore_signal(barrier, inc=1, device_id=partner, device_id_type=MESH)

    greet({"exp": mate})
    greet({"exp": cross})
    for r in range(len(siblings)):
        if siblings[r] == (0, 1):
            greet(sibling(r))
        else:
            pl.when(lead)(functools.partial(lambda r: greet(sibling(r)), r))
    pl.when(lead & (z > 0))(lambda: greet({"tok_0": z - 1}))
    pl.when(lead & (z < nz - 1))(lambda: greet({"tok_0": z + 1}))
    greeted = (
        2
        + nx
        + jnp.where(lead & (z > 0), 1, 0)
        + jnp.where(lead & (z < nz - 1), 1, 0)
    ).astype(I32)

    ids_copy.wait()
    digits = lax.broadcasted_iota(I32, (16, 8, width), 0)

    @pl.loop(0, chunks)
    def _(c):
        at = pl.ds(pl.multiple_of(c * width, width), width)
        ids = ids_v[:, at]
        hi, lo = ids >> 4, ids & 15
        hot_hi[:, at] = jnp.where(hi[None] == digits, 1.0, 0.0).reshape(128, width).astype(BF16)
        hot_lo[:, at] = jnp.where(lo[None] == digits, 1.0, 0.0).reshape(128, width).astype(BF16)

    pairs = lax.dot_general(
        hot_hi[...], hot_lo[...], (((1,), (1,)), ((), ())), preferred_element_type=F32
    )
    row = lax.broadcasted_iota(I32, (128, 128), 0)
    col = lax.broadcasted_iota(I32, (128, 128), 1)
    by_slot = jnp.where((row & 7) == (col & 7), pairs, 0.0).reshape(16, 8, 128).sum(axis=1)
    fold = jnp.where((row >> 3) == (col & 15), 1.0, 0.0).astype(BF16)
    upper = jnp.floor(by_slot * (1.0 / 64.0))
    lower = by_slot - 64.0 * upper
    counts = 64.0 * jnp.dot(upper.astype(BF16), fold, preferred_element_type=F32) + jnp.dot(
        lower.astype(BF16), fold, preferred_element_type=F32
    )
    sub = lax.broadcasted_iota(I32, (8, 128), 0)
    lane = lax.broadcasted_iota(I32, (8, 128), 1)
    pick = (lane >> 4) == sub
    first = jnp.sum(jnp.where(pick, counts[:8], 0.0), axis=0, keepdims=True)
    second = jnp.sum(jnp.where(pick, counts[8:], 0.0), axis=0, keepdims=True)
    d0[...] = jnp.where(sub == 0, first, jnp.where(sub == 1, second, 0.0))

    w_copy.wait()
    x_copy(1).start()
    wt_v[...] = w_v[...].T

    low_a = jnp.where((m == 0) | (m == 3), 1, 0)
    low_b = jnp.where(m < 2, 2, 0)
    pos_a = jnp.where(m < 2, 0, 1)
    pos_b = jnp.where(even_y, 0, 1)

    def part(c, block, second_half):
        return p_v[c, pl.ds(pl.multiple_of(block * own + second_half * half, half), half), :]

    def compute(c):
        p_v[c] = lax.dot_general(
            wt_v[...], x_v[c], (((1,), (1,)), ((), ())), preferred_element_type=F32
        )
        sa1[c, :half] = encode(part(c, low_a, 0)).astype(I16)
        sa1[c, half:] = encode(part(c, 3 - low_a, 0)).astype(I16)
        sb1[c, :half] = encode(part(c, low_b, 1)).astype(I16)
        sb1[c, half:] = encode(part(c, low_b + 1, 1)).astype(I16)

    def choose(c):
        ids = ids_v[:, pl.ds(pl.multiple_of(c * width, width), width)]
        tile, within = ids >> 3, ids & 7
        chosen = jnp.zeros((8, width), F32)
        for k in range(4 * own // 8):
            rows = p_v[c, 8 * k : 8 * k + 8, :]
            got = jnp.take_along_axis(rows, within, axis=0, mode="promise_in_bounds")
            chosen = jnp.where(tile == k, got, chosen)
        code = encode(chosen)
        sc1[c] = jnp.concatenate(
            [code[:, 128 * i : 128 * (i + 1)] for i in range(width // 128)], axis=0
        ).astype(I16)

    def remote(src, dst, c, kind, partner):
        return pltpu.make_async_remote_copy(
            src_ref=src.at[c],
            dst_ref=dst.at[c],
            send_sem=ss.at[kind, c],
            recv_sem=rs.at[kind, c],
            device_id={"exp": partner},
            device_id_type=MESH,
        )

    def even(c):
        return jnp.where(lax.rem(c, 2) == 0, mate, cross)

    def odd(c):
        return jnp.where(lax.rem(c, 2) == 0, cross, mate)

    def copies_ab(c):
        return remote(sa1, ra1, c, 0, mate), remote(sb1, rb1, c, 1, cross)

    def copy_c(c):
        return remote(sc1, rc1, c, 2, even(c))

    def copies_1(c):
        return (*copies_ab(c), copy_c(c))

    def copies_2(c):
        return (
            remote(sa2, ra2, c, 3, cross),
            remote(sb2, rb2, c, 4, mate),
            remote(sc2, rc2, c, 5, odd(c)),
        )

    def send(copies):
        for copy in copies:
            copy.start()

    def stage_1(c):
        compute(c)
        send(copies_ab(c))
        choose(c)
        copy_c(c).start()

    def count_copy(src, dst, r, sems, partner):
        return pltpu.make_async_remote_copy(
            src_ref=src, dst_ref=dst.at[r], send_sem=sems[0].at[r], recv_sem=sems[1].at[r],
            device_id=partner, device_id_type=MESH,
        )

    def near_copy(r):
        return count_copy(d0, near_by, r, (near_ss, near_rs), sibling(r))

    def down_copy(r):
        return count_copy(d1, above, r, (down_ss, down_rs), {"tok_0": z - r - 1})

    def up_copy(i):
        src = (d1, u1, u2)[i]
        return count_copy(src, below, i, (up_ss, up_rs), {"tok_0": z + (1, 2, 4)[i]})

    def tell(sem, there):
        pl.semaphore_signal(sem, inc=1, device_id={"tok_0": there}, device_id_type=MESH)

    def when_lower(action):
        for r in range(nz - 1):
            pl.when(lead & (z > r))(functools.partial(action, r))

    def when_upper(action):
        for r in range(nz - 1):
            pl.when(lead & (z + r + 1 < nz))(functools.partial(action, r))

    def near_sends(action):
        for r in range(len(siblings)):
            pl.when(core == 1 - siblings[r][1])(functools.partial(action, r))

    def hand_over():
        return pltpu.make_async_remote_copy(
            src_ref=total, dst_ref=total, send_sem=o_sem.at[0], recv_sem=o_sem.at[1],
            device_id={"tok_2": 1 - core}, device_id_type=MESH,
        )

    def bias_copy_to(src, dst, i, partner):
        return pltpu.make_async_remote_copy(
            src_ref=src, dst_ref=dst, send_sem=b_ss.at[i], recv_sem=b_rs.at[i],
            device_id={"exp": partner}, device_id_type=MESH,
        )

    x_copy(0).wait()
    x_copy(2).start()
    compute(0)
    pl.semaphore_wait(barrier, greeted)
    send(copies_ab(0))
    near_sends(lambda r: near_copy(r).start())
    x_copy(3).start()
    choose(0)
    copy_c(0).start()

    bias_copy.wait()
    mine = bias_v[...]
    mine = jnp.broadcast_to(jnp.concatenate([mine, mine], axis=1), (8, 128))
    my_row = jnp.where(m < 2, 0, 1)
    b0[...] = jnp.where((sub == my_row) & ((lane >> 6) == pos_b), mine, 0.0)


    x_copy(1).wait()
    x_copy(4).start()
    stage_1(1)
    bias_copy_to(b0, br1, 0, mate).start()

    def later(c):
        x_copy(c).wait()

        @pl.when(c + 3 < chunks)
        def _():
            x_copy(c + 3).start()

        stage_1(c)

    pl.loop(2, chunks)(later)

    pl.when(lead & (z > 0))(lambda: pl.semaphore_wait(wave, 1))
    pl.when(lead & (z < nz - 1))(lambda: tell(wave, z + 1))

    bias_copy_to(b0, br1, 0, mate).wait_recv()
    b1[...] = b0[...] + br1[...]
    bias_copy_to(b1, br2, 1, cross).start()

    def combine(c):
        for copy in copies_1(c):
            copy.wait_recv()
        at_a = pl.multiple_of(pos_a * half, half)
        at_b = pl.multiple_of(pos_b * half, half)
        off_a = pl.multiple_of((1 - pos_a) * half, half)
        off_b = pl.multiple_of((1 - pos_b) * half, half)
        sa2[c] = encode(part(c, cross, 0) + decode(ra1[c, pl.ds(off_a, half), :])).astype(I16)
        sb2[c] = encode(part(c, mate, 1) + decode(rb1[c, pl.ds(off_b, half), :])).astype(I16)
        sc2[c] = encode(decode(sc1[c]) + decode(rc1[c])).astype(I16)
        acc_v[c, :half] = part(c, m, 0) + decode(ra1[c, pl.ds(at_a, half), :])
        acc_v[c, half:] = part(c, m, 1) + decode(rb1[c, pl.ds(at_b, half), :])
        send(copies_2(c))

    pl.loop(0, 3)(combine)

    @pl.when(lead)
    def _():
        for r in range(len(siblings)):
            near_copy(r).wait_recv()
        d1[...] = sum((near_by[r] for r in range(len(siblings))), d0[...])

    when_lower(lambda r: down_copy(r).start())
    pl.when(lead & (z + 1 < nz))(lambda: up_copy(0).start())
    pl.when(lead & (z >= 1))(lambda: tell(crest_1, z - 1))

    pl.loop(3, 6)(combine)

    pl.when(lead & (z >= 1))(lambda: up_copy(0).wait_recv())

    @pl.when(lead)
    def _():
        u1[...] = d1[...] + jnp.where(z >= 1, below[0], 0.0)

    pl.when(lead & (z + 1 < nz))(lambda: pl.semaphore_wait(crest_1, 1))
    pl.when(lead & (z + 2 < nz))(lambda: up_copy(1).start())
    pl.when(lead & (z >= 2))(lambda: tell(crest_2, z - 2))

    pl.loop(6, chunks)(combine)

    def finish(c):
        for copy in copies_2(c):
            copy.wait_recv()
        at = pl.multiple_of(c * width, width)
        aff_ref[:half, pl.ds(at, width)] = sigmoid(acc_v[c, :half] + decode(ra2[c]))
        aff_ref[half:, pl.ds(at, width)] = sigmoid(acc_v[c, half:] + decode(rb2[c]))
        chosen = sigmoid(decode(sc2[c]) + decode(rc2[c]))
        for i in range(width // 128):
            values = chosen[8 * i : 8 * i + 8]
            total = jnp.sum(values, axis=0, keepdims=True)
            wts_ref[:, pl.ds(pl.multiple_of(at + 128 * i, 128), 128)] = 2.5 * values / total

    pl.loop(0, 3)(finish)

    pl.when(lead & (z >= 2))(lambda: up_copy(1).wait_recv())

    @pl.when(lead)
    def _():
        u2[...] = u1[...] + jnp.where(z >= 2, below[1], 0.0)

    pl.when(lead & (z + 2 < nz))(lambda: pl.semaphore_wait(crest_2, 1))
    pl.when(lead & (z + 4 < nz))(lambda: up_copy(2).start())

    pl.loop(3, chunks)(finish)

    pl.when(lead & (z >= 4))(lambda: up_copy(2).wait_recv())
    when_upper(lambda r: down_copy(r).wait_recv())

    @pl.when(lead)
    def _():
        load = u2[...] + jnp.where(z >= 4, below[2], 0.0)
        for r in range(nz - 1):
            load = load + jnp.where(z + r + 1 < nz, above[r], 0.0)
        total[...] = load
        hand_over().start()

    pl.when(core == 0)(lambda: hand_over().wait_recv())
    bias_copy_to(b1, br2, 1, cross).wait_recv()
    load = total[...]
    gap = target - (4.0 * own) * load
    sign = jnp.where(gap > 0.0, 1.0, jnp.where(gap < 0.0, -1.0, 0.0))
    new_bias = (b1[...] + br2[...]) + 0.001 * sign
    for i in range(2):
        load_ref[:, 128 * i : 128 * (i + 1)] = load[i : i + 1]
        new_ref[:, 128 * i : 128 * (i + 1)] = new_bias[i : i + 1]

    @pl.loop(0, chunks)
    def _(c):
        for copy in (*copies_1(c), *copies_2(c)):
            copy.wait_send()

    near_sends(lambda r: near_copy(r).wait_send())
    pl.when(lead)(lambda: hand_over().wait_send())
    when_lower(lambda r: down_copy(r).wait_send())
    pl.when(lead & (z + 1 < nz))(lambda: up_copy(0).wait_send())
    pl.when(lead & (z + 2 < nz))(lambda: up_copy(1).wait_send())
    pl.when(lead & (z + 4 < nz))(lambda: up_copy(2).wait_send())
    bias_copy_to(b0, br1, 0, mate).wait_send()
    bias_copy_to(b1, br2, 1, cross).wait_send()


def hand_out(*refs):
    count = len(refs) // 2
    copies = [
        pltpu.make_async_copy(refs[i], refs[count + i], refs[-1].at[i]) for i in range(count)
    ]
    for copy in copies:
        copy.start()
    for copy in copies:
        copy.wait()


def local(shape, tokens, gate_weight, expert_ids, expert_bias):
    nz, nx, nc = shape
    rows, depth = tokens.shape
    experts = gate_weight.shape[1]
    slots = expert_ids.shape[1]
    width = 256
    chunks = rows // width
    own = experts // 4
    target = float(rows * nz * nx * nc * slots)
    sizes = (nz, nx, nc, chunks, width, target)
    dma = pltpu.SemaphoreType.DMA
    big = pltpu.VMEM((chunks, own, width), I16)
    small = pltpu.VMEM((chunks, own // 2, width), I16)
    few = pltpu.VMEM((chunks, 16, 128), I16)
    tile = pltpu.VMEM((8, 128), F32)

    def tiles(n):
        return pltpu.VMEM((n, 8, 128), F32)

    group, line = nx * nc - 1, nz - 1
    made = pl.pallas_call(
        functools.partial(kernel, sizes),
        out_shape=(
            pltpu.VMEM((own, rows), F32),
            pltpu.VMEM((slots, rows), F32),
            pltpu.VMEM((1, experts), F32),
            pltpu.VMEM((1, experts), F32),
        ),
        in_specs=[pl.BlockSpec(memory_space=pltpu.HBM)] * 4,
        out_specs=(pl.BlockSpec(memory_space=pltpu.VMEM),) * 4,
        scratch_shapes=[
            pltpu.VMEM((chunks, width, depth), BF16),
            pltpu.VMEM((depth, experts), BF16),
            pltpu.VMEM((experts, depth), BF16),
            pltpu.VMEM((slots, rows), I32),
            pltpu.VMEM((1, own), F32),
            pltpu.VMEM((chunks, experts, width), F32),
            pltpu.VMEM((chunks, own, width), F32),
            big, big, small, small, few, few, big, big, small, small, few, few,
            pltpu.VMEM((128, rows), BF16), pltpu.VMEM((128, rows), BF16),
            tile, tile, tile, tile, tile, tiles(group), tiles(line), tiles(3), tile, tile, tile, tile,
            dma((chunks,)), dma((3,)), dma((6, chunks)), dma((6, chunks)),
            dma((group,)), dma((group,)), dma((line,)), dma((line,)), dma((3,)), dma((3,)),
            dma((2,)), dma((2,)), dma((2,)), *[pltpu.SemaphoreType.REGULAR] * 3,
        ],
        compiler_params=pltpu.CompilerParams(
            collective_id=0, has_side_effects=True, vmem_limit_bytes=66300000
        ),
        name="router",
    )(tokens, gate_weight, expert_ids.T, expert_bias.reshape(1, own))
    aff, wts, load, new = pl.pallas_call(
        hand_out,
        out_shape=tuple(jax.ShapeDtypeStruct(a.shape, a.dtype) for a in made),
        in_specs=[pl.BlockSpec(memory_space=pltpu.VMEM)] * 4,
        out_specs=(pl.BlockSpec(memory_space=pltpu.HBM),) * 4,
        scratch_shapes=[dma((4,))],
        compiler_params=pltpu.CompilerParams(vmem_limit_bytes=2**20),
        name="hand_out",
    )(*made)
    return aff.T, wts.T, load.reshape(experts), new.reshape(experts)


def solution(mesh):
    shape = (8, 4, 2)
    split = Mesh(mesh.devices.reshape(*shape, mesh.shape["exp"]), (*TOK, "exp"))
    in_specs = (P(TOK, "exp"), P("exp", None), P(TOK, None), P("exp"))
    out_specs = (P(TOK, "exp"), P(TOK, None), P(), P())
    return jax.shard_map(
        functools.partial(local, shape),
        mesh=split, in_specs=in_specs, out_specs=out_specs, check_vma=False,
    )
```

```python
import functools

import jax
import jax.numpy as jnp
from jax import lax
from jax.experimental import pallas as pl
from jax.experimental.pallas import tpu as pltpu
from jax.sharding import Mesh
from jax.sharding import PartitionSpec as P

TOK = ("tok_0", "tok_1", "tok_2")
MESH = pl.DeviceIdType.MESH
F32 = jnp.float32
BF16 = jnp.bfloat16
I32 = jnp.int32
I16 = jnp.int16

STEPS = 3800.0
KNEE = 0.25


def encode(x):
    grade = jnp.log(jnp.abs(x) * (1.0 / KNEE) + 1.0) * STEPS + 0.5
    return jnp.where(x < 0.0, -grade, grade).astype(I32)


def decode(code):
    grade = code.astype(I32).astype(F32)
    size = jnp.exp(jnp.abs(grade) * (1.0 / STEPS)) * KNEE - KNEE
    return jnp.where(grade < 0.0, -size, size)


def sigmoid(x):
    return 1.0 / (1.0 + jnp.exp(-x))


def kernel(
    sizes, x_hbm, w_hbm, ids_hbm, bias_hbm, aff_ref, wts_ref, load_ref, new_ref,
    x_v, w_v, wt_v, ids_v, bias_v, p_v, acc_v,
    sa1, sb1, sa2, sb2, sc1, sc2, ra1, rb1, ra2, rb2, rc1, rc2,
    hot_hi, hot_lo, d0, d1, u1, u2, total, near_by, above, below, b0, b1, br1, br2,
    x_sem, in_sem, ss, rs, near_ss, near_rs, down_ss, down_rs, up_ss, up_rs, b_ss, b_rs, o_sem, crest_1, crest_2,
):
    nz, nx, nc, chunks, width, target = sizes
    own = 64
    half = own // 2
    z, xx, core, m = (lax.axis_index(a) for a in (*TOK, "exp"))
    even_y = lax.rem(m, 2) == 0
    mate = jnp.where(even_y, m + 1, m - 1)
    cross = 3 - m
    lead = core == 1
    siblings = [(dx, dc) for dx in range(nx) for dc in range(nc)][1:]

    def turned(at, by, length):
        there = at + by
        return jnp.where(there >= length, there - length, there)

    def sibling(r):
        dx, dc = siblings[r]
        return {"tok_1": turned(xx, dx, nx), "tok_2": turned(core, dc, nc)}

    def x_copy(c):
        return pltpu.make_async_copy(
            x_hbm.at[pl.ds(pl.multiple_of(c * width, width), width), :], x_v.at[c], x_sem.at[c]
        )

    ids_copy = pltpu.make_async_copy(ids_hbm, ids_v, in_sem.at[0])
    w_copy = pltpu.make_async_copy(w_hbm, w_v, in_sem.at[1])
    bias_copy = pltpu.make_async_copy(bias_hbm, bias_v, in_sem.at[2])
    ids_copy.start()
    w_copy.start()
    x_copy(0).start()
    bias_copy.start()

    barrier = pltpu.get_barrier_semaphore()

    def greet(partner):
        pl.semaphore_signal(barrier, inc=1, device_id=partner, device_id_type=MESH)

    greet({"exp": mate})
    greet({"exp": cross})
    for r in range(len(siblings)):
        if siblings[r] == (0, 1):
            greet(sibling(r))
        else:
            pl.when(lead)(functools.partial(lambda r: greet(sibling(r)), r))
    pl.when(lead & (z > 0))(lambda: greet({"tok_0": z - 1}))
    for r in range(nz - 1):
        pl.when(lead & (z + r + 1 < nz))(
            functools.partial(lambda r: greet({"tok_0": z + r + 1}), r)
        )
    greeted = (
        2
        + nx
        + jnp.where(lead, z, 0)
        + jnp.where(lead & (z < nz - 1), 1, 0)
    ).astype(I32)

    ids_copy.wait()
    digits = lax.broadcasted_iota(I32, (16, 8, width), 0)

    @pl.loop(0, chunks)
    def _(c):
        at = pl.ds(pl.multiple_of(c * width, width), width)
        ids = ids_v[:, at]
        hi, lo = ids >> 4, ids & 15
        hot_hi[:, at] = jnp.where(hi[None] == digits, 1.0, 0.0).reshape(128, width).astype(BF16)
        hot_lo[:, at] = jnp.where(lo[None] == digits, 1.0, 0.0).reshape(128, width).astype(BF16)

    pairs = lax.dot_general(
        hot_hi[...], hot_lo[...], (((1,), (1,)), ((), ())), preferred_element_type=F32
    )
    row = lax.broadcasted_iota(I32, (128, 128), 0)
    col = lax.broadcasted_iota(I32, (128, 128), 1)
    by_slot = jnp.where((row & 7) == (col & 7), pairs, 0.0).reshape(16, 8, 128).sum(axis=1)
    fold = jnp.where((row >> 3) == (col & 15), 1.0, 0.0).astype(BF16)
    upper = jnp.floor(by_slot * (1.0 / 64.0))
    lower = by_slot - 64.0 * upper
    counts = 64.0 * jnp.dot(upper.astype(BF16), fold, preferred_element_type=F32) + jnp.dot(
        lower.astype(BF16), fold, preferred_element_type=F32
    )
    sub = lax.broadcasted_iota(I32, (8, 128), 0)
    lane = lax.broadcasted_iota(I32, (8, 128), 1)
    pick = (lane >> 4) == sub
    first = jnp.sum(jnp.where(pick, counts[:8], 0.0), axis=0, keepdims=True)
    second = jnp.sum(jnp.where(pick, counts[8:], 0.0), axis=0, keepdims=True)
    d0[...] = jnp.where(sub == 0, first, jnp.where(sub == 1, second, 0.0))

    w_copy.wait()
    x_copy(1).start()
    wt_v[...] = w_v[...].T

    low_a = jnp.where((m == 0) | (m == 3), 1, 0)
    low_b = jnp.where(m < 2, 2, 0)
    pos_a = jnp.where(m < 2, 0, 1)
    pos_b = jnp.where(even_y, 0, 1)

    def part(c, block, second_half):
        return p_v[c, pl.ds(pl.multiple_of(block * own + second_half * half, half), half), :]

    def compute(c):
        p_v[c] = lax.dot_general(
            wt_v[...], x_v[c], (((1,), (1,)), ((), ())), preferred_element_type=F32
        )
        sa1[c, :half] = encode(part(c, low_a, 0)).astype(I16)
        sa1[c, half:] = encode(part(c, 3 - low_a, 0)).astype(I16)
        sb1[c, :half] = encode(part(c, low_b, 1)).astype(I16)
        sb1[c, half:] = encode(part(c, low_b + 1, 1)).astype(I16)

    def choose(c):
        ids = ids_v[:, pl.ds(pl.multiple_of(c * width, width), width)]
        tile, within = ids >> 3, ids & 7
        chosen = jnp.zeros((8, width), F32)
        for k in range(4 * own // 8):
            rows = p_v[c, 8 * k : 8 * k + 8, :]
            got = jnp.take_along_axis(rows, within, axis=0, mode="promise_in_bounds")
            chosen = jnp.where(tile == k, got, chosen)
        code = encode(chosen)
        sc1[c] = jnp.concatenate(
            [code[:, 128 * i : 128 * (i + 1)] for i in range(width // 128)], axis=0
        ).astype(I16)

    def remote(src, dst, c, kind, partner):
        return pltpu.make_async_remote_copy(
            src_ref=src.at[c],
            dst_ref=dst.at[c],
            send_sem=ss.at[kind, c],
            recv_sem=rs.at[kind, c],
            device_id={"exp": partner},
            device_id_type=MESH,
        )

    def even(c):
        return jnp.where(lax.rem(c, 2) == 0, mate, cross)

    def odd(c):
        return jnp.where(lax.rem(c, 2) == 0, cross, mate)

    def copies_ab(c):
        return remote(sa1, ra1, c, 0, mate), remote(sb1, rb1, c, 1, cross)

    def copy_c(c):
        return remote(sc1, rc1, c, 2, even(c))

    def copies_1(c):
        return (*copies_ab(c), copy_c(c))

    def copies_2(c):
        return (
            remote(sa2, ra2, c, 3, cross),
            remote(sb2, rb2, c, 4, mate),
            remote(sc2, rc2, c, 5, odd(c)),
        )

    def send(copies):
        for copy in copies:
            copy.start()

    def stage_1(c):
        compute(c)
        send(copies_ab(c))
        choose(c)
        copy_c(c).start()

    def count_copy(src, dst, r, sems, partner):
        return pltpu.make_async_remote_copy(
            src_ref=src, dst_ref=dst.at[r], send_sem=sems[0].at[r], recv_sem=sems[1].at[r],
            device_id=partner, device_id_type=MESH,
        )

    def near_copy(r):
        return count_copy(d0, near_by, r, (near_ss, near_rs), sibling(r))

    def down_copy(r):
        return count_copy(d1, above, r, (down_ss, down_rs), {"tok_0": z - r - 1})

    def up_copy(i):
        src = (d1, u1, u2)[i]
        return count_copy(src, below, i, (up_ss, up_rs), {"tok_0": z + (1, 2, 4)[i]})

    def tell(sem, there):
        pl.semaphore_signal(sem, inc=1, device_id={"tok_0": there}, device_id_type=MESH)

    def when_lower(action):
        for r in range(nz - 1):
            pl.when(lead & (z > r))(functools.partial(action, r))

    def when_upper(action):
        for r in range(nz - 1):
            pl.when(lead & (z + r + 1 < nz))(functools.partial(action, r))

    def near_sends(action):
        for r in range(len(siblings)):
            pl.when(core == 1 - siblings[r][1])(functools.partial(action, r))

    def hand_over():
        return pltpu.make_async_remote_copy(
            src_ref=total, dst_ref=total, send_sem=o_sem.at[0], recv_sem=o_sem.at[1],
            device_id={"tok_2": 1 - core}, device_id_type=MESH,
        )

    def bias_copy_to(src, dst, i, partner):
        return pltpu.make_async_remote_copy(
            src_ref=src, dst_ref=dst, send_sem=b_ss.at[i], recv_sem=b_rs.at[i],
            device_id={"exp": partner}, device_id_type=MESH,
        )

    x_copy(0).wait()
    x_copy(2).start()
    compute(0)
    pl.semaphore_wait(barrier, greeted)
    send(copies_ab(0))
    near_sends(lambda r: near_copy(r).start())
    x_copy(3).start()
    choose(0)
    copy_c(0).start()

    bias_copy.wait()
    mine = bias_v[...]
    mine = jnp.broadcast_to(jnp.concatenate([mine, mine], axis=1), (8, 128))
    my_row = jnp.where(m < 2, 0, 1)
    b0[...] = jnp.where((sub == my_row) & ((lane >> 6) == pos_b), mine, 0.0)


    x_copy(1).wait()
    x_copy(4).start()
    stage_1(1)
    bias_copy_to(b0, br1, 0, mate).start()

    def later(c):
        x_copy(c).wait()

        @pl.when(c + 3 < chunks)
        def _():
            x_copy(c + 3).start()

        stage_1(c)

    pl.loop(2, chunks - 1)(later)

    @pl.when(lead)
    def _():
        for r in range(len(siblings)):
            near_copy(r).wait_recv()
        d1[...] = sum((near_by[r] for r in range(len(siblings))), d0[...])

    when_lower(lambda r: down_copy(r).start())
    pl.when(lead & (z + 1 < nz))(lambda: up_copy(0).start())
    pl.when(lead & (z >= 1))(lambda: tell(crest_1, z - 1))

    pl.loop(chunks - 1, chunks)(later)

    bias_copy_to(b0, br1, 0, mate).wait_recv()
    b1[...] = b0[...] + br1[...]
    bias_copy_to(b1, br2, 1, cross).start()

    def combine(c):
        for copy in copies_1(c):
            copy.wait_recv()
        at_a = pl.multiple_of(pos_a * half, half)
        at_b = pl.multiple_of(pos_b * half, half)
        off_a = pl.multiple_of((1 - pos_a) * half, half)
        off_b = pl.multiple_of((1 - pos_b) * half, half)
        sa2[c] = encode(part(c, cross, 0) + decode(ra1[c, pl.ds(off_a, half), :])).astype(I16)
        sb2[c] = encode(part(c, mate, 1) + decode(rb1[c, pl.ds(off_b, half), :])).astype(I16)
        sc2[c] = encode(decode(sc1[c]) + decode(rc1[c])).astype(I16)
        acc_v[c, :half] = part(c, m, 0) + decode(ra1[c, pl.ds(at_a, half), :])
        acc_v[c, half:] = part(c, m, 1) + decode(rb1[c, pl.ds(at_b, half), :])
        send(copies_2(c))

    pl.loop(0, 4)(combine)

    pl.when(lead & (z >= 1))(lambda: up_copy(0).wait_recv())

    @pl.when(lead)
    def _():
        u1[...] = d1[...] + jnp.where(z >= 1, below[0], 0.0)

    pl.when(lead & (z + 1 < nz))(lambda: pl.semaphore_wait(crest_1, 1))
    pl.when(lead & (z + 2 < nz))(lambda: up_copy(1).start())
    pl.when(lead & (z >= 2))(lambda: tell(crest_2, z - 2))

    pl.loop(4, chunks - 1)(combine)

    pl.when(lead & (z >= 2))(lambda: up_copy(1).wait_recv())

    @pl.when(lead)
    def _():
        u2[...] = u1[...] + jnp.where(z >= 2, below[1], 0.0)

    pl.when(lead & (z + 2 < nz))(lambda: pl.semaphore_wait(crest_2, 1))
    pl.when(lead & (z + 4 < nz))(lambda: up_copy(2).start())

    pl.loop(chunks - 1, chunks)(combine)

    def finish(c):
        for copy in copies_2(c):
            copy.wait_recv()
        at = pl.multiple_of(c * width, width)
        aff_ref[:half, pl.ds(at, width)] = sigmoid(acc_v[c, :half] + decode(ra2[c]))
        aff_ref[half:, pl.ds(at, width)] = sigmoid(acc_v[c, half:] + decode(rb2[c]))
        chosen = sigmoid(decode(sc2[c]) + decode(rc2[c]))
        for i in range(width // 128):
            values = chosen[8 * i : 8 * i + 8]
            total = jnp.sum(values, axis=0, keepdims=True)
            wts_ref[:, pl.ds(pl.multiple_of(at + 128 * i, 128), 128)] = 2.5 * values / total

    pl.loop(0, 6)(finish)

    pl.when(lead & (z >= 4))(lambda: up_copy(2).wait_recv())
    when_upper(lambda r: down_copy(r).wait_recv())

    @pl.when(lead)
    def _():
        load = u2[...] + jnp.where(z >= 4, below[2], 0.0)
        for r in range(nz - 1):
            load = load + jnp.where(z + r + 1 < nz, above[r], 0.0)
        total[...] = load
        hand_over().start()

    pl.loop(6, chunks)(finish)

    pl.when(core == 0)(lambda: hand_over().wait_recv())
    bias_copy_to(b1, br2, 1, cross).wait_recv()
    load = total[...]
    gap = target - (4.0 * own) * load
    sign = jnp.where(gap > 0.0, 1.0, jnp.where(gap < 0.0, -1.0, 0.0))
    new_bias = (b1[...] + br2[...]) + 0.001 * sign
    for i in range(2):
        load_ref[:, 128 * i : 128 * (i + 1)] = load[i : i + 1]
        new_ref[:, 128 * i : 128 * (i + 1)] = new_bias[i : i + 1]

    @pl.loop(0, chunks)
    def _(c):
        for copy in (*copies_1(c), *copies_2(c)):
            copy.wait_send()

    near_sends(lambda r: near_copy(r).wait_send())
    pl.when(lead)(lambda: hand_over().wait_send())
    when_lower(lambda r: down_copy(r).wait_send())
    pl.when(lead & (z + 1 < nz))(lambda: up_copy(0).wait_send())
    pl.when(lead & (z + 2 < nz))(lambda: up_copy(1).wait_send())
    pl.when(lead & (z + 4 < nz))(lambda: up_copy(2).wait_send())
    bias_copy_to(b0, br1, 0, mate).wait_send()
    bias_copy_to(b1, br2, 1, cross).wait_send()


def hand_out(*refs):
    count = len(refs) // 2
    copies = [
        pltpu.make_async_copy(refs[i], refs[count + i], refs[-1].at[i]) for i in range(count)
    ]
    for copy in copies:
        copy.start()
    for copy in copies:
        copy.wait()


def local(shape, tokens, gate_weight, expert_ids, expert_bias):
    nz, nx, nc = shape
    rows, depth = tokens.shape
    experts = gate_weight.shape[1]
    slots = expert_ids.shape[1]
    width = 256
    chunks = rows // width
    own = experts // 4
    target = float(rows * nz * nx * nc * slots)
    sizes = (nz, nx, nc, chunks, width, target)
    dma = pltpu.SemaphoreType.DMA
    big = pltpu.VMEM((chunks, own, width), I16)
    small = pltpu.VMEM((chunks, own // 2, width), I16)
    few = pltpu.VMEM((chunks, 16, 128), I16)
    tile = pltpu.VMEM((8, 128), F32)

    def tiles(n):
        return pltpu.VMEM((n, 8, 128), F32)

    group, line = nx * nc - 1, nz - 1
    made = pl.pallas_call(
        functools.partial(kernel, sizes),
        out_shape=(
            pltpu.VMEM((own, rows), F32),
            pltpu.VMEM((slots, rows), F32),
            pltpu.VMEM((1, experts), F32),
            pltpu.VMEM((1, experts), F32),
        ),
        in_specs=[pl.BlockSpec(memory_space=pltpu.HBM)] * 4,
        out_specs=(pl.BlockSpec(memory_space=pltpu.VMEM),) * 4,
        scratch_shapes=[
            pltpu.VMEM((chunks, width, depth), BF16),
            pltpu.VMEM((depth, experts), BF16),
            pltpu.VMEM((experts, depth), BF16),
            pltpu.VMEM((slots, rows), I32),
            pltpu.VMEM((1, own), F32),
            pltpu.VMEM((chunks, experts, width), F32),
            pltpu.VMEM((chunks, own, width), F32),
            big, big, small, small, few, few, big, big, small, small, few, few,
            pltpu.VMEM((128, rows), BF16), pltpu.VMEM((128, rows), BF16),
            tile, tile, tile, tile, tile, tiles(group), tiles(line), tiles(3), tile, tile, tile, tile,
            dma((chunks,)), dma((3,)), dma((6, chunks)), dma((6, chunks)),
            dma((group,)), dma((group,)), dma((line,)), dma((line,)), dma((3,)), dma((3,)),
            dma((2,)), dma((2,)), dma((2,)), *[pltpu.SemaphoreType.REGULAR] * 2,
        ],
        compiler_params=pltpu.CompilerParams(
            collective_id=0, has_side_effects=True, vmem_limit_bytes=66300000
        ),
        name="router",
    )(tokens, gate_weight, expert_ids.T, expert_bias.reshape(1, own))
    aff, wts, load, new = pl.pallas_call(
        hand_out,
        out_shape=tuple(jax.ShapeDtypeStruct(a.shape, a.dtype) for a in made),
        in_specs=[pl.BlockSpec(memory_space=pltpu.VMEM)] * 4,
        out_specs=(pl.BlockSpec(memory_space=pltpu.HBM),) * 4,
        scratch_shapes=[dma((4,))],
        compiler_params=pltpu.CompilerParams(vmem_limit_bytes=2**20),
        name="hand_out",
    )(*made)
    return aff.T, wts.T, load.reshape(experts), new.reshape(experts)


def solution(mesh):
    shape = (8, 4, 2)
    split = Mesh(mesh.devices.reshape(*shape, mesh.shape["exp"]), (*TOK, "exp"))
    in_specs = (P(TOK, "exp"), P("exp", None), P(TOK, None), P("exp"))
    out_specs = (P(TOK, "exp"), P(TOK, None), P(), P())
    return jax.shard_map(
        functools.partial(local, shape),
        mesh=split, in_specs=in_specs, out_specs=out_specs, check_vma=False,
    )
```

```python
import functools

import jax
import jax.numpy as jnp
from jax import lax
from jax.experimental import pallas as pl
from jax.experimental.pallas import tpu as pltpu
from jax.sharding import Mesh
from jax.sharding import PartitionSpec as P

TOK = ("tok_0", "tok_1", "tok_2")
MESH = pl.DeviceIdType.MESH
F32 = jnp.float32
BF16 = jnp.bfloat16
I32 = jnp.int32
I16 = jnp.int16

STEPS = 3800.0
KNEE = 0.25


def encode(x):
    grade = jnp.log(jnp.abs(x) * (1.0 / KNEE) + 1.0) * STEPS + 0.5
    return jnp.where(x < 0.0, -grade, grade).astype(I32)


def decode(code):
    grade = code.astype(I32).astype(F32)
    size = jnp.exp(jnp.abs(grade) * (1.0 / STEPS)) * KNEE - KNEE
    return jnp.where(grade < 0.0, -size, size)


def sigmoid(x):
    return 1.0 / (1.0 + jnp.exp(-x))


def kernel(
    sizes, x_hbm, w_hbm, ids_hbm, bias_hbm, aff_ref, wts_ref, load_ref, new_ref,
    x_v, w_v, wt_v, ids_v, bias_v, p_v, acc_v,
    sa1, sb1, sa2, sb2, sc1, sc2, r1, r2, rc1, rc2,
    hot_hi, hot_lo, d0, d1, u1, u2, total, near_by, above, below, b0, b1, br1, br2,
    x_sem, in_sem, ss, rs1, rs2, rsc, near_sem, down_sem, up_ss, up_rs, b_ss, b_rs, o_sem, crest_1, crest_2,
):
    nz, nx, nc, chunks, width, target = sizes
    own = 64
    half = own // 2
    z, xx, core, m = (lax.axis_index(a) for a in (*TOK, "exp"))
    even_y = lax.rem(m, 2) == 0
    mate = jnp.where(even_y, m + 1, m - 1)
    cross = 3 - m
    lead = core == 1
    siblings = [(dx, dc) for dx in range(nx) for dc in range(nc)][1:]

    def turned(at, by, length):
        there = at + by
        return jnp.where(there >= length, there - length, there)

    def sibling(r):
        dx, dc = siblings[r]
        return {"tok_1": turned(xx, dx, nx), "tok_2": turned(core, dc, nc)}

    def x_copy(c):
        return pltpu.make_async_copy(
            x_hbm.at[pl.ds(pl.multiple_of(c * width, width), width), :], x_v.at[c], x_sem.at[c]
        )

    ids_copy = pltpu.make_async_copy(ids_hbm, ids_v, in_sem.at[0])
    w_copy = pltpu.make_async_copy(w_hbm, w_v, in_sem.at[1])
    bias_copy = pltpu.make_async_copy(bias_hbm, bias_v, in_sem.at[2])
    ids_copy.start()
    w_copy.start()
    x_copy(0).start()
    bias_copy.start()

    barrier = pltpu.get_barrier_semaphore()

    def greet(partner):
        pl.semaphore_signal(barrier, inc=1, device_id=partner, device_id_type=MESH)

    greet({"exp": mate})
    greet({"exp": cross})
    for r in range(len(siblings)):
        if siblings[r] == (0, 1):
            greet(sibling(r))
        else:
            pl.when(lead)(functools.partial(lambda r: greet(sibling(r)), r))
    pl.when(lead & (z > 0))(lambda: greet({"tok_0": z - 1}))
    for r in range(nz - 1):
        pl.when(lead & (z + r + 1 < nz))(
            functools.partial(lambda r: greet({"tok_0": z + r + 1}), r)
        )
    greeted = (
        2
        + nx
        + jnp.where(lead, z, 0)
        + jnp.where(lead & (z < nz - 1), 1, 0)
    ).astype(I32)

    ids_copy.wait()
    digits = lax.broadcasted_iota(I32, (16, 8, width), 0)

    @pl.loop(0, chunks)
    def _(c):
        at = pl.ds(pl.multiple_of(c * width, width), width)
        ids = ids_v[:, at]
        hi, lo = ids >> 4, ids & 15
        hot_hi[:, at] = jnp.where(hi[None] == digits, 1.0, 0.0).reshape(128, width).astype(BF16)
        hot_lo[:, at] = jnp.where(lo[None] == digits, 1.0, 0.0).reshape(128, width).astype(BF16)

    pairs = lax.dot_general(
        hot_hi[...], hot_lo[...], (((1,), (1,)), ((), ())), preferred_element_type=F32
    )
    row = lax.broadcasted_iota(I32, (128, 128), 0)
    col = lax.broadcasted_iota(I32, (128, 128), 1)
    by_slot = jnp.where((row & 7) == (col & 7), pairs, 0.0).reshape(16, 8, 128).sum(axis=1)
    fold = jnp.where((row >> 3) == (col & 15), 1.0, 0.0).astype(BF16)
    upper = jnp.floor(by_slot * (1.0 / 64.0))
    lower = by_slot - 64.0 * upper
    counts = 64.0 * jnp.dot(upper.astype(BF16), fold, preferred_element_type=F32) + jnp.dot(
        lower.astype(BF16), fold, preferred_element_type=F32
    )
    sub = lax.broadcasted_iota(I32, (8, 128), 0)
    lane = lax.broadcasted_iota(I32, (8, 128), 1)
    pick = (lane >> 4) == sub
    first = jnp.sum(jnp.where(pick, counts[:8], 0.0), axis=0, keepdims=True)
    second = jnp.sum(jnp.where(pick, counts[8:], 0.0), axis=0, keepdims=True)
    d0[...] = jnp.where(sub == 0, first, jnp.where(sub == 1, second, 0.0))

    w_copy.wait()
    x_copy(1).start()
    wt_v[...] = w_v[...].T

    low_a = jnp.where((m == 0) | (m == 3), 1, 0)
    low_b = jnp.where(m < 2, 2, 0)
    pos_a = jnp.where(m < 2, 0, 1)
    pos_b = jnp.where(even_y, 0, 1)

    def part(c, block, second_half):
        return p_v[c, pl.ds(pl.multiple_of(block * own + second_half * half, half), half), :]

    def compute(c):
        p_v[c] = lax.dot_general(
            wt_v[...], x_v[c], (((1,), (1,)), ((), ())), preferred_element_type=F32
        )
        sa1[c, :half] = encode(part(c, low_a, 0)).astype(I16)
        sa1[c, half:] = encode(part(c, 3 - low_a, 0)).astype(I16)
        sb1[c, :half] = encode(part(c, low_b, 1)).astype(I16)
        sb1[c, half:] = encode(part(c, low_b + 1, 1)).astype(I16)

    def choose(c):
        ids = ids_v[:, pl.ds(pl.multiple_of(c * width, width), width)]
        tile, within = ids >> 3, ids & 7
        chosen = jnp.zeros((8, width), F32)
        for k in range(4 * own // 8):
            rows = p_v[c, 8 * k : 8 * k + 8, :]
            got = jnp.take_along_axis(rows, within, axis=0, mode="promise_in_bounds")
            chosen = jnp.where(tile == k, got, chosen)
        code = encode(chosen)
        sc1[c] = jnp.concatenate(
            [code[:, 128 * i : 128 * (i + 1)] for i in range(width // 128)], axis=0
        ).astype(I16)

    def remote(src, dst, send_sem, recv_sem, partner):
        return pltpu.make_async_remote_copy(
            src_ref=src, dst_ref=dst, send_sem=send_sem, recv_sem=recv_sem,
            device_id={"exp": partner}, device_id_type=MESH,
        )

    def even(c):
        return jnp.where(lax.rem(c, 2) == 0, mate, cross)

    def odd(c):
        return jnp.where(lax.rem(c, 2) == 0, cross, mate)

    def copies_ab(c):
        return (
            remote(sa1.at[c], r1.at[c, pl.ds(0, own)], ss.at[0], rs1.at[c], mate),
            remote(sb1.at[c], r1.at[c, pl.ds(own, own)], ss.at[1], rs1.at[c], cross),
        )

    def copy_c(c):
        return remote(sc1.at[c], rc1.at[c], ss.at[2], rsc.at[0], even(c))

    def copies_2(c):
        return (
            remote(sa2.at[c], r2.at[c, pl.ds(0, half)], ss.at[3], rs2.at[c], cross),
            remote(sb2.at[c], r2.at[c, pl.ds(half, half)], ss.at[4], rs2.at[c], mate),
        )

    def copy_c2(c):
        return remote(sc2.at[c], rc2.at[c], ss.at[5], rsc.at[1], odd(c))

    def arrived(dst, recv_sem):
        remote(dst, dst, ss.at[0], recv_sem, mate).wait_recv()

    def left(src, i):
        remote(src, src, ss.at[i], rsc.at[0], mate).wait_send()

    def send(copies):
        for copy in copies:
            copy.start()

    def stage_1(c):
        compute(c)
        send(copies_ab(c))
        choose(c)
        copy_c(c).start()

    def count_copy(src, dst, r, sems, partner):
        return pltpu.make_async_remote_copy(
            src_ref=src, dst_ref=dst.at[r], send_sem=sems[0], recv_sem=sems[1],
            device_id=partner, device_id_type=MESH,
        )

    def near_copy(r):
        return count_copy(d0, near_by, r, (near_sem.at[0], near_sem.at[1]), sibling(r))

    def down_copy(r):
        return count_copy(d1, above, r, (down_sem.at[0], down_sem.at[1]), {"tok_0": z - r - 1})

    def up_copy(i):
        src = (d1, u1, u2)[i]
        return count_copy(src, below, i, (up_ss.at[i], up_rs.at[i]), {"tok_0": z + (1, 2, 4)[i]})

    def tell(sem, there):
        pl.semaphore_signal(sem, inc=1, device_id={"tok_0": there}, device_id_type=MESH)

    def when_lower(action):
        for r in range(nz - 1):
            pl.when(lead & (z > r))(functools.partial(action, r))

    def tiles_of(ref, n, sems):
        return remote(ref.at[pl.ds(0, n)], ref.at[pl.ds(0, n)], sems.at[0], sems.at[1], mate)

    def down_arrived():
        for n in range(1, nz):
            pl.when(lead & (z == nz - 1 - n))(
                functools.partial(lambda n: tiles_of(above, n, down_sem).wait_recv(), n)
            )

    def down_left():
        for n in range(1, nz):
            pl.when(lead & (z == n))(
                functools.partial(lambda n: tiles_of(above, n, down_sem).wait_send(), n)
            )

    def near_sends(action):
        for r in range(len(siblings)):
            pl.when(core == 1 - siblings[r][1])(functools.partial(action, r))

    def hand_over():
        return pltpu.make_async_remote_copy(
            src_ref=total, dst_ref=total, send_sem=o_sem.at[0], recv_sem=o_sem.at[1],
            device_id={"tok_2": 1 - core}, device_id_type=MESH,
        )

    def bias_copy_to(src, dst, i, partner):
        return pltpu.make_async_remote_copy(
            src_ref=src, dst_ref=dst, send_sem=b_ss.at[i], recv_sem=b_rs.at[i],
            device_id={"exp": partner}, device_id_type=MESH,
        )

    x_copy(0).wait()
    x_copy(2).start()
    compute(0)
    pl.semaphore_wait(barrier, greeted)
    send(copies_ab(0))
    near_sends(lambda r: near_copy(r).start())
    x_copy(3).start()
    choose(0)
    copy_c(0).start()

    bias_copy.wait()
    mine = bias_v[...]
    mine = jnp.broadcast_to(jnp.concatenate([mine, mine], axis=1), (8, 128))
    my_row = jnp.where(m < 2, 0, 1)
    b0[...] = jnp.where((sub == my_row) & ((lane >> 6) == pos_b), mine, 0.0)


    x_copy(1).wait()
    x_copy(4).start()
    stage_1(1)
    bias_copy_to(b0, br1, 0, mate).start()

    def later(c):
        x_copy(c).wait()

        @pl.when(c + 3 < chunks)
        def _():
            x_copy(c + 3).start()

        stage_1(c)

    pl.loop(2, chunks - 1)(later)

    @pl.when(lead)
    def _():
        tiles_of(near_by, len(siblings), near_sem).wait_recv()
        d1[...] = sum((near_by[r] for r in range(len(siblings))), d0[...])

    when_lower(lambda r: down_copy(r).start())
    pl.when(lead & (z + 1 < nz))(lambda: up_copy(0).start())
    pl.when(lead & (z >= 1))(lambda: tell(crest_1, z - 1))

    pl.loop(chunks - 1, chunks)(later)

    bias_copy_to(b0, br1, 0, mate).wait_recv()
    b1[...] = b0[...] + br1[...]
    bias_copy_to(b1, br2, 1, cross).start()

    at_a = pl.ds(pl.multiple_of(pos_a * half, half), half)
    off_a = pl.ds(pl.multiple_of((1 - pos_a) * half, half), half)
    at_b = pl.ds(pl.multiple_of(own + pos_b * half, half), half)
    off_b = pl.ds(pl.multiple_of(own + (1 - pos_b) * half, half), half)

    def combine(c):
        arrived(r1.at[c], rs1.at[c])
        sa2[c] = encode(part(c, cross, 0) + decode(r1[c, off_a, :])).astype(I16)
        sb2[c] = encode(part(c, mate, 1) + decode(r1[c, off_b, :])).astype(I16)
        acc_v[c, :half] = part(c, m, 0) + decode(r1[c, at_a, :])
        acc_v[c, half:] = part(c, m, 1) + decode(r1[c, at_b, :])
        send(copies_2(c))

    pl.loop(0, 4)(combine)

    pl.when(lead & (z >= 1))(lambda: up_copy(0).wait_recv())

    @pl.when(lead)
    def _():
        u1[...] = d1[...] + jnp.where(z >= 1, below[0], 0.0)

    pl.when(lead & (z + 1 < nz))(lambda: pl.semaphore_wait(crest_1, 1))
    pl.when(lead & (z + 2 < nz))(lambda: up_copy(1).start())
    pl.when(lead & (z >= 2))(lambda: tell(crest_2, z - 2))

    pl.loop(4, chunks)(combine)

    arrived(rc1, rsc.at[0])
    for c in range(chunks):
        sc2[c] = encode(decode(sc1[c]) + decode(rc1[c])).astype(I16)
    for c in range(chunks):
        copy_c2(c).start()

    def finish(c):
        arrived(r2.at[c], rs2.at[c])
        at = pl.ds(pl.multiple_of(c * width, width), width)
        aff_ref[:half, at] = sigmoid(acc_v[c, :half] + decode(r2[c, :half]))
        aff_ref[half:, at] = sigmoid(acc_v[c, half:] + decode(r2[c, half:]))

    pl.loop(0, 2)(finish)

    pl.when(lead & (z >= 2))(lambda: up_copy(1).wait_recv())

    @pl.when(lead)
    def _():
        u2[...] = u1[...] + jnp.where(z >= 2, below[1], 0.0)

    pl.when(lead & (z + 2 < nz))(lambda: pl.semaphore_wait(crest_2, 1))
    pl.when(lead & (z + 4 < nz))(lambda: up_copy(2).start())

    pl.loop(2, 6)(finish)

    pl.when(lead & (z >= 4))(lambda: up_copy(2).wait_recv())
    down_arrived()

    @pl.when(lead)
    def _():
        load = u2[...] + jnp.where(z >= 4, below[2], 0.0)
        for r in range(nz - 1):
            load = load + jnp.where(z + r + 1 < nz, above[r], 0.0)
        total[...] = load
        hand_over().start()

    pl.loop(6, chunks)(finish)

    arrived(rc2, rsc.at[1])
    for c in range(chunks):
        chosen = sigmoid(decode(sc2[c]) + decode(rc2[c]))
        for i in range(width // 128):
            values = chosen[8 * i : 8 * i + 8]
            at = pl.ds(c * width + 128 * i, 128)
            wts_ref[:, at] = 2.5 * values / jnp.sum(values, axis=0, keepdims=True)

    pl.when(core == 0)(lambda: hand_over().wait_recv())
    bias_copy_to(b1, br2, 1, cross).wait_recv()
    load = total[...]
    gap = target - (4.0 * own) * load
    sign = jnp.where(gap > 0.0, 1.0, jnp.where(gap < 0.0, -1.0, 0.0))
    new_bias = (b1[...] + br2[...]) + 0.001 * sign
    for i in range(2):
        load_ref[:, 128 * i : 128 * (i + 1)] = load[i : i + 1]
        new_ref[:, 128 * i : 128 * (i + 1)] = new_bias[i : i + 1]

    for i, src in enumerate((sa1, sb1, sc1, sa2, sb2, sc2)):
        left(src, i)
    pl.when(core == 0)(lambda: tiles_of(near_by, nx, near_sem).wait_send())
    if nx > 1:
        pl.when(lead)(lambda: tiles_of(near_by, nx - 1, near_sem).wait_send())
    pl.when(lead)(lambda: hand_over().wait_send())
    down_left()
    pl.when(lead & (z + 1 < nz))(lambda: up_copy(0).wait_send())
    pl.when(lead & (z + 2 < nz))(lambda: up_copy(1).wait_send())
    pl.when(lead & (z + 4 < nz))(lambda: up_copy(2).wait_send())
    bias_copy_to(b0, br1, 0, mate).wait_send()
    bias_copy_to(b1, br2, 1, cross).wait_send()


def hand_out(*refs):
    count = len(refs) // 2
    copies = [
        pltpu.make_async_copy(refs[i], refs[count + i], refs[-1].at[i]) for i in range(count)
    ]
    for copy in copies:
        copy.start()
    for copy in copies:
        copy.wait()


def local(shape, tokens, gate_weight, expert_ids, expert_bias):
    nz, nx, nc = shape
    rows, depth = tokens.shape
    experts = gate_weight.shape[1]
    slots = expert_ids.shape[1]
    width = 256
    chunks = rows // width
    own = experts // 4
    target = float(rows * nz * nx * nc * slots)
    sizes = (nz, nx, nc, chunks, width, target)
    dma = pltpu.SemaphoreType.DMA
    big = pltpu.VMEM((chunks, own, width), I16)
    small = pltpu.VMEM((chunks, own // 2, width), I16)
    few = pltpu.VMEM((chunks, 16, 128), I16)
    tile = pltpu.VMEM((8, 128), F32)

    def tiles(n):
        return pltpu.VMEM((n, 8, 128), F32)

    group, line = nx * nc - 1, nz - 1
    made = pl.pallas_call(
        functools.partial(kernel, sizes),
        out_shape=(
            pltpu.VMEM((own, rows), F32),
            pltpu.VMEM((slots, rows), F32),
            pltpu.VMEM((1, experts), F32),
            pltpu.VMEM((1, experts), F32),
        ),
        in_specs=[pl.BlockSpec(memory_space=pltpu.HBM)] * 4,
        out_specs=(pl.BlockSpec(memory_space=pltpu.VMEM),) * 4,
        scratch_shapes=[
            pltpu.VMEM((chunks, width, depth), BF16),
            pltpu.VMEM((depth, experts), BF16),
            pltpu.VMEM((experts, depth), BF16),
            pltpu.VMEM((slots, rows), I32),
            pltpu.VMEM((1, own), F32),
            pltpu.VMEM((chunks, experts, width), F32),
            pltpu.VMEM((chunks, own, width), F32),
            big, big, small, small, few, few,
            pltpu.VMEM((chunks, 2 * own, width), I16), pltpu.VMEM((chunks, own, width), I16), few, few,
            pltpu.VMEM((128, rows), BF16), pltpu.VMEM((128, rows), BF16),
            tile, tile, tile, tile, tile, tiles(group), tiles(line), tiles(3), tile, tile, tile, tile,
            dma((chunks,)), dma((3,)), dma((6,)), dma((chunks,)), dma((chunks,)), dma((2,)),
            dma((2,)), dma((2,)), dma((3,)), dma((3,)),
            dma((2,)), dma((2,)), dma((2,)), *[pltpu.SemaphoreType.REGULAR] * 2,
        ],
        compiler_params=pltpu.CompilerParams(
            collective_id=0, has_side_effects=True, vmem_limit_bytes=66300000
        ),
        name="router",
    )(tokens, gate_weight, expert_ids.T, expert_bias.reshape(1, own))
    aff, wts, load, new = pl.pallas_call(
        hand_out,
        out_shape=tuple(jax.ShapeDtypeStruct(a.shape, a.dtype) for a in made),
        in_specs=[pl.BlockSpec(memory_space=pltpu.VMEM)] * 4,
        out_specs=(pl.BlockSpec(memory_space=pltpu.HBM),) * 4,
        scratch_shapes=[dma((4,))],
        compiler_params=pltpu.CompilerParams(vmem_limit_bytes=2**20),
        name="hand_out",
    )(*made)
    return aff.T, wts.T, load.reshape(experts), new.reshape(experts)


def solution(mesh):
    shape = (8, 4, 2)
    split = Mesh(mesh.devices.reshape(*shape, mesh.shape["exp"]), (*TOK, "exp"))
    in_specs = (P(TOK, "exp"), P("exp", None), P(TOK, None), P("exp"))
    out_specs = (P(TOK, "exp"), P(TOK, None), P(), P())
    return jax.shard_map(
        functools.partial(local, shape),
        mesh=split, in_specs=in_specs, out_specs=out_specs, check_vma=False,
    )
```

```python
import functools

import jax
import jax.numpy as jnp
from jax import lax
from jax.experimental import pallas as pl
from jax.experimental.pallas import tpu as pltpu
from jax.sharding import Mesh
from jax.sharding import PartitionSpec as P

TOK = ("tok_0", "tok_1", "tok_2")
MESH = pl.DeviceIdType.MESH
F32 = jnp.float32
BF16 = jnp.bfloat16
I32 = jnp.int32
I16 = jnp.int16

STEPS = 3800.0
KNEE = 0.25


def encode(x):
    grade = jnp.log(jnp.abs(x) * (1.0 / KNEE) + 1.0) * STEPS + 0.5
    return jnp.where(x < 0.0, -grade, grade).astype(I32)


def decode(code):
    grade = code.astype(I32).astype(F32)
    size = jnp.exp(jnp.abs(grade) * (1.0 / STEPS)) * KNEE - KNEE
    return jnp.where(grade < 0.0, -size, size)


def sigmoid(x):
    return 1.0 / (1.0 + jnp.exp(-x))


def kernel(
    sizes, x_hbm, w_hbm, ids_hbm, bias_hbm, aff_ref, wts_ref, load_ref, new_ref,
    x_v, w_v, wt_v, ids_v, bias_v, p_v, acc_v,
    sa1, sb1, sa2, sb2, sc1, sc2, r1, r2, rc1, rc2,
    hot_hi, hot_lo, d0, d1, u1, u2, total, near_by, above, below, b0, b1, br1, br2,
    x_sem, in_sem, ss, rs1, rs2, rsc, near_sem, down_sem, up_ss, up_rs, b_ss, b_rs, o_sem, crest_1, crest_2,
):
    nz, nx, nc, chunks, width, target = sizes
    own = 64
    half = own // 2
    z, xx, core, m = (lax.axis_index(a) for a in (*TOK, "exp"))
    even_y = lax.rem(m, 2) == 0
    mate = jnp.where(even_y, m + 1, m - 1)
    cross = 3 - m
    lead = core == 1
    siblings = [(dx, dc) for dx in range(nx) for dc in range(nc)][1:]

    def turned(at, by, length):
        there = at + by
        return jnp.where(there >= length, there - length, there)

    def sibling(r):
        dx, dc = siblings[r]
        return {"tok_1": turned(xx, dx, nx), "tok_2": turned(core, dc, nc)}

    def x_copy(c):
        return pltpu.make_async_copy(
            x_hbm.at[pl.ds(pl.multiple_of(c * width, width), width), :], x_v.at[c], x_sem.at[c]
        )

    ids_copy = pltpu.make_async_copy(ids_hbm, ids_v, in_sem.at[0])
    w_copy = pltpu.make_async_copy(w_hbm, w_v, in_sem.at[1])
    bias_copy = pltpu.make_async_copy(bias_hbm, bias_v, in_sem.at[2])
    ids_copy.start()
    w_copy.start()
    x_copy(0).start()
    bias_copy.start()

    barrier = pltpu.get_barrier_semaphore()

    def greet(partner):
        pl.semaphore_signal(barrier, inc=1, device_id=partner, device_id_type=MESH)

    greet({"exp": mate})
    greet({"exp": cross})
    for r in range(len(siblings)):
        if siblings[r] == (0, 1):
            greet(sibling(r))
        else:
            pl.when(lead)(functools.partial(lambda r: greet(sibling(r)), r))
    pl.when(lead & (z > 0))(lambda: greet({"tok_0": z - 1}))
    for r in range(nz - 1):
        pl.when(lead & (z + r + 1 < nz))(
            functools.partial(lambda r: greet({"tok_0": z + r + 1}), r)
        )
    greeted = (
        2
        + nx
        + jnp.where(lead, z, 0)
        + jnp.where(lead & (z < nz - 1), 1, 0)
    ).astype(I32)

    ids_copy.wait()
    digits = lax.broadcasted_iota(I32, (16, 8, width), 0)

    @pl.loop(0, chunks)
    def _(c):
        at = pl.ds(pl.multiple_of(c * width, width), width)
        ids = ids_v[:, at]
        hi, lo = ids >> 4, ids & 15
        hot_hi[:, at] = jnp.where(hi[None] == digits, 1.0, 0.0).reshape(128, width).astype(BF16)
        hot_lo[:, at] = jnp.where(lo[None] == digits, 1.0, 0.0).reshape(128, width).astype(BF16)

    pairs = lax.dot_general(
        hot_hi[...], hot_lo[...], (((1,), (1,)), ((), ())), preferred_element_type=F32
    )
    row = lax.broadcasted_iota(I32, (128, 128), 0)
    col = lax.broadcasted_iota(I32, (128, 128), 1)
    by_slot = jnp.where((row & 7) == (col & 7), pairs, 0.0).reshape(16, 8, 128).sum(axis=1)
    fold = jnp.where((row >> 3) == (col & 15), 1.0, 0.0).astype(BF16)
    upper = jnp.floor(by_slot * (1.0 / 64.0))
    lower = by_slot - 64.0 * upper
    counts = 64.0 * jnp.dot(upper.astype(BF16), fold, preferred_element_type=F32) + jnp.dot(
        lower.astype(BF16), fold, preferred_element_type=F32
    )
    sub = lax.broadcasted_iota(I32, (8, 128), 0)
    lane = lax.broadcasted_iota(I32, (8, 128), 1)
    pick = (lane >> 4) == sub
    first = jnp.sum(jnp.where(pick, counts[:8], 0.0), axis=0, keepdims=True)
    second = jnp.sum(jnp.where(pick, counts[8:], 0.0), axis=0, keepdims=True)
    d0[...] = jnp.where(sub == 0, first, jnp.where(sub == 1, second, 0.0))

    w_copy.wait()
    x_copy(1).start()
    x_copy(2).start()
    wt_v[...] = w_v[...].T

    low_a = jnp.where((m == 0) | (m == 3), 1, 0)
    low_b = jnp.where(m < 2, 2, 0)
    pos_a = jnp.where(m < 2, 0, 1)
    pos_b = jnp.where(even_y, 0, 1)

    def part(c, block, second_half):
        return p_v[c, pl.ds(pl.multiple_of(block * own + second_half * half, half), half), :]

    def compute(c):
        p_v[c] = lax.dot_general(
            wt_v[...], x_v[c], (((1,), (1,)), ((), ())), preferred_element_type=F32
        )
        sa1[c, :half] = encode(part(c, low_a, 0)).astype(I16)
        sa1[c, half:] = encode(part(c, 3 - low_a, 0)).astype(I16)
        sb1[c, :half] = encode(part(c, low_b, 1)).astype(I16)
        sb1[c, half:] = encode(part(c, low_b + 1, 1)).astype(I16)

    def choose(c):
        ids = ids_v[:, pl.ds(pl.multiple_of(c * width, width), width)]
        tile, within = ids >> 3, ids & 7
        chosen = jnp.zeros((8, width), F32)
        for k in range(4 * own // 8):
            rows = p_v[c, 8 * k : 8 * k + 8, :]
            got = jnp.take_along_axis(rows, within, axis=0, mode="promise_in_bounds")
            chosen = jnp.where(tile == k, got, chosen)
        code = encode(chosen)
        sc1[c] = jnp.concatenate(
            [code[:, 128 * i : 128 * (i + 1)] for i in range(width // 128)], axis=0
        ).astype(I16)

    def remote(src, dst, send_sem, recv_sem, partner):
        return pltpu.make_async_remote_copy(
            src_ref=src, dst_ref=dst, send_sem=send_sem, recv_sem=recv_sem,
            device_id={"exp": partner}, device_id_type=MESH,
        )

    def even(c):
        return jnp.where(lax.rem(c, 2) == 0, mate, cross)

    def odd(c):
        return jnp.where(lax.rem(c, 2) == 0, cross, mate)

    def copies_ab(c):
        return (
            remote(sa1.at[c], r1.at[c, pl.ds(0, own)], ss.at[0], rs1.at[c], mate),
            remote(sb1.at[c], r1.at[c, pl.ds(own, own)], ss.at[1], rs1.at[c], cross),
        )

    def copy_c(c):
        return remote(sc1.at[c], rc1.at[c], ss.at[2], rsc.at[0], even(c))

    def copies_2(c):
        return (
            remote(sa2.at[c], r2.at[c, pl.ds(0, half)], ss.at[3], rs2.at[c], cross),
            remote(sb2.at[c], r2.at[c, pl.ds(half, half)], ss.at[4], rs2.at[c], mate),
        )

    def copy_c2(c):
        return remote(sc2.at[c], rc2.at[c], ss.at[5], rsc.at[1], odd(c))

    def arrived(dst, recv_sem):
        remote(dst, dst, ss.at[0], recv_sem, mate).wait_recv()

    def left(src, i):
        remote(src, src, ss.at[i], rsc.at[0], mate).wait_send()

    def send(copies):
        for copy in copies:
            copy.start()

    def stage_1(c):
        compute(c)
        send(copies_ab(c))
        choose(c)
        copy_c(c).start()

    def count_copy(src, dst, r, sems, partner):
        return pltpu.make_async_remote_copy(
            src_ref=src, dst_ref=dst.at[r], send_sem=sems[0], recv_sem=sems[1],
            device_id=partner, device_id_type=MESH,
        )

    def near_copy(r):
        return count_copy(d0, near_by, r, (near_sem.at[0], near_sem.at[1]), sibling(r))

    def down_copy(r):
        return count_copy(d1, above, r, (down_sem.at[0], down_sem.at[1]), {"tok_0": z - r - 1})

    def up_copy(i):
        src = (d1, u1, u2)[i]
        return count_copy(src, below, i, (up_ss.at[i], up_rs.at[i]), {"tok_0": z + (1, 2, 4)[i]})

    def tell(sem, there):
        pl.semaphore_signal(sem, inc=1, device_id={"tok_0": there}, device_id_type=MESH)

    def when_lower(action):
        for r in range(nz - 1):
            pl.when(lead & (z > r))(functools.partial(action, r))

    def tiles_of(ref, n, sems):
        return remote(ref.at[pl.ds(0, n)], ref.at[pl.ds(0, n)], sems.at[0], sems.at[1], mate)

    def down_arrived():
        for n in range(1, nz):
            pl.when(lead & (z == nz - 1 - n))(
                functools.partial(lambda n: tiles_of(above, n, down_sem).wait_recv(), n)
            )

    def down_left():
        for n in range(1, nz):
            pl.when(lead & (z == n))(
                functools.partial(lambda n: tiles_of(above, n, down_sem).wait_send(), n)
            )

    def near_sends(action):
        for r in range(len(siblings)):
            pl.when(core == 1 - siblings[r][1])(functools.partial(action, r))

    def hand_over():
        return pltpu.make_async_remote_copy(
            src_ref=total, dst_ref=total, send_sem=o_sem.at[0], recv_sem=o_sem.at[1],
            device_id={"tok_2": 1 - core}, device_id_type=MESH,
        )

    def bias_copy_to(src, dst, i, partner):
        return pltpu.make_async_remote_copy(
            src_ref=src, dst_ref=dst, send_sem=b_ss.at[i], recv_sem=b_rs.at[i],
            device_id={"exp": partner}, device_id_type=MESH,
        )

    @pl.loop(0, chunks)
    def _(c):
        x_copy(c).wait()

        @pl.when(c + 3 < chunks)
        def _():
            x_copy(c + 3).start()

        compute(c)
        pl.when(c == 0)(lambda: pl.semaphore_wait(barrier, greeted))
        send(copies_ab(c))

        @pl.when(c == 0)
        def _():
            near_sends(lambda r: near_copy(r).start())
            bias_copy.wait()
            mine = bias_v[...]
            mine = jnp.broadcast_to(jnp.concatenate([mine, mine], axis=1), (8, 128))
            my_row = jnp.where(m < 2, 0, 1)
            b0[...] = jnp.where((sub == my_row) & ((lane >> 6) == pos_b), mine, 0.0)
            bias_copy_to(b0, br1, 0, mate).start()

        choose(c)
        copy_c(c).start()

    @pl.when(lead)
    def _():
        tiles_of(near_by, len(siblings), near_sem).wait_recv()
        d1[...] = sum((near_by[r] for r in range(len(siblings))), d0[...])

    when_lower(lambda r: down_copy(r).start())
    pl.when(lead & (z + 1 < nz))(lambda: up_copy(0).start())
    pl.when(lead & (z >= 1))(lambda: tell(crest_1, z - 1))

    bias_copy_to(b0, br1, 0, mate).wait_recv()
    b1[...] = b0[...] + br1[...]
    bias_copy_to(b1, br2, 1, cross).start()

    at_a = pl.ds(pl.multiple_of(pos_a * half, half), half)
    off_a = pl.ds(pl.multiple_of((1 - pos_a) * half, half), half)
    at_b = pl.ds(pl.multiple_of(own + pos_b * half, half), half)
    off_b = pl.ds(pl.multiple_of(own + (1 - pos_b) * half, half), half)

    def combine(c):
        arrived(r1.at[c], rs1.at[c])
        sa2[c] = encode(part(c, cross, 0) + decode(r1[c, off_a, :])).astype(I16)
        sb2[c] = encode(part(c, mate, 1) + decode(r1[c, off_b, :])).astype(I16)
        acc_v[c, :half] = part(c, m, 0) + decode(r1[c, at_a, :])
        acc_v[c, half:] = part(c, m, 1) + decode(r1[c, at_b, :])
        send(copies_2(c))

    def second_step():
        pl.when(lead & (z >= 1))(lambda: up_copy(0).wait_recv())

        @pl.when(lead)
        def _():
            u1[...] = d1[...] + jnp.where(z >= 1, below[0], 0.0)

        pl.when(lead & (z + 1 < nz))(lambda: pl.semaphore_wait(crest_1, 1))
        pl.when(lead & (z + 2 < nz))(lambda: up_copy(1).start())
        pl.when(lead & (z >= 2))(lambda: tell(crest_2, z - 2))

    @pl.loop(0, chunks)
    def _(c):
        combine(c)
        pl.when(c == 3)(second_step)

    arrived(rc1, rsc.at[0])
    for c in range(chunks):
        sc2[c] = encode(decode(sc1[c]) + decode(rc1[c])).astype(I16)
    for c in range(chunks):
        copy_c2(c).start()

    def finish(c):
        arrived(r2.at[c], rs2.at[c])
        at = pl.ds(pl.multiple_of(c * width, width), width)
        aff_ref[:half, at] = sigmoid(acc_v[c, :half] + decode(r2[c, :half]))
        aff_ref[half:, at] = sigmoid(acc_v[c, half:] + decode(r2[c, half:]))

    def third_step():
        pl.when(lead & (z >= 2))(lambda: up_copy(1).wait_recv())

        @pl.when(lead)
        def _():
            u2[...] = u1[...] + jnp.where(z >= 2, below[1], 0.0)

        pl.when(lead & (z + 2 < nz))(lambda: pl.semaphore_wait(crest_2, 1))
        pl.when(lead & (z + 4 < nz))(lambda: up_copy(2).start())

    def sum_up():
        pl.when(lead & (z >= 4))(lambda: up_copy(2).wait_recv())
        down_arrived()

        @pl.when(lead)
        def _():
            load = u2[...] + jnp.where(z >= 4, below[2], 0.0)
            for r in range(nz - 1):
                load = load + jnp.where(z + r + 1 < nz, above[r], 0.0)
            total[...] = load
            hand_over().start()

    @pl.loop(0, chunks)
    def _(c):
        finish(c)
        pl.when(c == 0)(third_step)
        pl.when(c == chunks - 1)(sum_up)

    arrived(rc2, rsc.at[1])
    for c in range(chunks):
        chosen = sigmoid(decode(sc2[c]) + decode(rc2[c]))
        for i in range(width // 128):
            values = chosen[8 * i : 8 * i + 8]
            at = pl.ds(c * width + 128 * i, 128)
            wts_ref[:, at] = 2.5 * values / jnp.sum(values, axis=0, keepdims=True)

    pl.when(core == 0)(lambda: hand_over().wait_recv())
    bias_copy_to(b1, br2, 1, cross).wait_recv()
    load = total[...]
    gap = target - (4.0 * own) * load
    sign = jnp.where(gap > 0.0, 1.0, jnp.where(gap < 0.0, -1.0, 0.0))
    new_bias = (b1[...] + br2[...]) + 0.001 * sign
    for i in range(2):
        load_ref[:, 128 * i : 128 * (i + 1)] = load[i : i + 1]
        new_ref[:, 128 * i : 128 * (i + 1)] = new_bias[i : i + 1]

    for i, src in enumerate((sa1, sb1, sc1, sa2, sb2, sc2)):
        left(src, i)
    pl.when(core == 0)(lambda: tiles_of(near_by, nx, near_sem).wait_send())
    if nx > 1:
        pl.when(lead)(lambda: tiles_of(near_by, nx - 1, near_sem).wait_send())
    pl.when(lead)(lambda: hand_over().wait_send())
    down_left()
    pl.when(lead & (z + 1 < nz))(lambda: up_copy(0).wait_send())
    pl.when(lead & (z + 2 < nz))(lambda: up_copy(1).wait_send())
    pl.when(lead & (z + 4 < nz))(lambda: up_copy(2).wait_send())
    bias_copy_to(b0, br1, 0, mate).wait_send()
    bias_copy_to(b1, br2, 1, cross).wait_send()


def hand_out(*refs):
    count = len(refs) // 2
    copies = [
        pltpu.make_async_copy(refs[i], refs[count + i], refs[-1].at[i]) for i in range(count)
    ]
    for copy in copies:
        copy.start()
    for copy in copies:
        copy.wait()


def local(shape, tokens, gate_weight, expert_ids, expert_bias):
    nz, nx, nc = shape
    rows, depth = tokens.shape
    experts = gate_weight.shape[1]
    slots = expert_ids.shape[1]
    width = 256
    chunks = rows // width
    own = experts // 4
    target = float(rows * nz * nx * nc * slots)
    sizes = (nz, nx, nc, chunks, width, target)
    dma = pltpu.SemaphoreType.DMA
    big = pltpu.VMEM((chunks, own, width), I16)
    small = pltpu.VMEM((chunks, own // 2, width), I16)
    few = pltpu.VMEM((chunks, 16, 128), I16)
    tile = pltpu.VMEM((8, 128), F32)

    def tiles(n):
        return pltpu.VMEM((n, 8, 128), F32)

    group, line = nx * nc - 1, nz - 1
    made = pl.pallas_call(
        functools.partial(kernel, sizes),
        out_shape=(
            pltpu.VMEM((own, rows), F32),
            pltpu.VMEM((slots, rows), F32),
            pltpu.VMEM((1, experts), F32),
            pltpu.VMEM((1, experts), F32),
        ),
        in_specs=[pl.BlockSpec(memory_space=pltpu.HBM)] * 4,
        out_specs=(pl.BlockSpec(memory_space=pltpu.VMEM),) * 4,
        scratch_shapes=[
            pltpu.VMEM((chunks, width, depth), BF16),
            pltpu.VMEM((depth, experts), BF16),
            pltpu.VMEM((experts, depth), BF16),
            pltpu.VMEM((slots, rows), I32),
            pltpu.VMEM((1, own), F32),
            pltpu.VMEM((chunks, experts, width), F32),
            pltpu.VMEM((chunks, own, width), F32),
            big, big, small, small, few, few,
            pltpu.VMEM((chunks, 2 * own, width), I16), pltpu.VMEM((chunks, own, width), I16), few, few,
            pltpu.VMEM((128, rows), BF16), pltpu.VMEM((128, rows), BF16),
            tile, tile, tile, tile, tile, tiles(group), tiles(line), tiles(3), tile, tile, tile, tile,
            dma((chunks,)), dma((3,)), dma((6,)), dma((chunks,)), dma((chunks,)), dma((2,)),
            dma((2,)), dma((2,)), dma((3,)), dma((3,)),
            dma((2,)), dma((2,)), dma((2,)), *[pltpu.SemaphoreType.REGULAR] * 2,
        ],
        compiler_params=pltpu.CompilerParams(
            collective_id=0, has_side_effects=True, vmem_limit_bytes=66300000
        ),
        name="router",
    )(tokens, gate_weight, expert_ids.T, expert_bias.reshape(1, own))
    aff, wts, load, new = pl.pallas_call(
        hand_out,
        out_shape=tuple(jax.ShapeDtypeStruct(a.shape, a.dtype) for a in made),
        in_specs=[pl.BlockSpec(memory_space=pltpu.VMEM)] * 4,
        out_specs=(pl.BlockSpec(memory_space=pltpu.HBM),) * 4,
        scratch_shapes=[dma((4,))],
        compiler_params=pltpu.CompilerParams(vmem_limit_bytes=2**20),
        name="hand_out",
    )(*made)
    return aff.T, wts.T, load.reshape(experts), new.reshape(experts)


def solution(mesh):
    shape = (8, 4, 2)
    split = Mesh(mesh.devices.reshape(*shape, mesh.shape["exp"]), (*TOK, "exp"))
    in_specs = (P(TOK, "exp"), P("exp", None), P(TOK, None), P("exp"))
    out_specs = (P(TOK, "exp"), P(TOK, None), P(), P())
    return jax.shard_map(
        functools.partial(local, shape),
        mesh=split, in_specs=in_specs, out_specs=out_specs, check_vma=False,
    )
```
